8 devices in a mesh: dp: 2 (over y, z), ep: 4 (over x, core).
Axes of the slice: x: 2, y: 2, z: 1, core: 2. Of those that a mesh axis runs over, the one named last changes fastest.
Arguments:
- x: bfloat16 [2, 4, 1024, 2048], P('dp', 'ep'), parts along dimension 0
- expert: int32 [2, 4, 1024, 4], P('dp', 'ep'), parts along dimension 0
- slot: int32 [2, 4, 1024, 4], P('dp', 'ep'), parts along dimension 0
- gate: float32 [2, 4, 1024, 4], P('dp', 'ep'), parts along dimension 0
- w_gate: bfloat16 [60, 2048, 1408], P('ep')
- w_up: bfloat16 [60, 2048, 1408], P('ep')
- w_down: bfloat16 [60, 1408, 2048], P('ep')
- s_gate: bfloat16 [2048, 5632], replicated
- s_up: bfloat16 [2048, 5632], replicated
- s_down: bfloat16 [5632, 2048], replicated
Outputs:
- y: bfloat16 [2, 4, 1024, 2048], P('dp', 'ep'), parts along dimension 0
There are 2 independent parts. The reference program is written for one: setup_inputs(seed, part) draws one part's arguments, and reference() takes and returns one part's arrays. A program takes and returns all parts, laid end to end along the dimension named above; an argument that names none is the same for every part.
All inputs are finite; a program needn't handle non-finite values.
Results may differ from the reference program's by a relative error of at most 0.009.
Values are sent between devices in bfloat16 or wider.
A program may use at most 2 GiB of HBM per device.

```python
import jax
import jax.numpy as jnp

MEMBERS = 4
TOKENS = 1024
D = 2048
FF = 1408
TOP = 4
EXPERTS = 60
SHARED_FF = 5632
SLOTS = 5 * TOKENS * TOP // (4 * EXPERTS)


def setup_inputs(seed: int = 0, part: int = 0) -> dict:
    own, k1, k2, k3, k4, k5, k6 = jax.random.split(jax.random.key(seed), 7)
    kx, ke, kl, kg = jax.random.split(jax.random.fold_in(own, part), 4)
    devices = (1, MEMBERS)
    place = jax.random.permutation(kl, jnp.arange(EXPERTS, dtype=jnp.uint32))
    slow = ((EXPERTS + (9 * place) % EXPERTS) << ((9 * place) // EXPERTS)) // EXPERTS
    wait = (jax.random.bits(ke, (*devices, TOKENS, EXPERTS), jnp.uint32) >> 10) * slow
    expert = jnp.argsort(wait, axis=-1)[..., :TOP].astype(jnp.int32)
    chosen = jax.nn.one_hot(expert, EXPERTS, dtype=jnp.int32)
    in_line = jnp.cumsum(chosen.reshape(*devices, TOKENS * TOP, EXPERTS), axis=2) - 1
    slot = jnp.sum(in_line.reshape(chosen.shape) * chosen, axis=-1)

    def one(key, rows, columns):
        return (jax.random.normal(key, (rows, columns), jnp.float32) * rows**-0.5).astype(jnp.bfloat16)

    def weights(key, rows, columns):
        return jax.lax.map(lambda k: one(k, rows, columns), jax.random.split(key, EXPERTS))

    return {
        "x": jax.random.normal(kx, (*devices, TOKENS, D), jnp.float32).astype(jnp.bfloat16),
        "expert": expert,
        "slot": slot,
        "gate": jax.nn.softmax(jax.random.normal(kg, expert.shape, jnp.float32)),
        "w_gate": weights(k1, D, FF),
        "w_up": weights(k2, D, FF),
        "w_down": weights(k3, FF, D),
        "s_gate": one(k4, D, SHARED_FF),
        "s_up": one(k5, D, SHARED_FF),
        "s_down": one(k6, SHARED_FF, D),
    }


def einsum(form, a, b):
    return jnp.einsum(form, a.astype(jnp.float32), b.astype(jnp.float32))


def for_all(x, s_gate, s_up, s_down):
    h = jax.nn.silu(einsum("...d,df->...f", x, s_gate)) * einsum("...d,df->...f", x, s_up)
    return einsum("...f,fd->...d", h.astype(jnp.bfloat16), s_down)


def reference(x, expert, slot, gate, w_gate, w_up, w_down, s_gate, s_up, s_down):
    to_expert = jax.nn.one_hot(expert, EXPERTS, dtype=jnp.bfloat16)
    to_slot = jax.nn.one_hot(slot, SLOTS, dtype=jnp.bfloat16)
    weighted = to_expert * gate[..., None].astype(jnp.bfloat16)
    dispatch = einsum("abtke,abtkc->abtec", to_expert, to_slot).astype(jnp.bfloat16)
    combine = einsum("abtke,abtkc->abtec", weighted, to_slot).astype(jnp.bfloat16)
    z = einsum("abtec,abtd->aebcd", dispatch, x).astype(jnp.bfloat16)
    h = jax.nn.silu(einsum("aebcd,edf->aebcf", z, w_gate))
    h = (h * einsum("aebcd,edf->aebcf", z, w_up)).astype(jnp.bfloat16)
    out = einsum("aebcf,efd->aebcd", h, w_down).astype(jnp.bfloat16)
    y = einsum("abtec,aebcd->abtd", combine, out)
    return (y + for_all(x, s_gate, s_up, s_down)).astype(jnp.bfloat16)
```

```python
import functools

import jax
import jax.numpy as jnp
from jax import lax
from jax.experimental import pallas as pl
from jax.experimental.pallas import tpu as pltpu
from jax.sharding import PartitionSpec as P


MIB = 1 << 20
ROW = 16
BLK = 128
F32, BF16 = jnp.float32, jnp.bfloat16


def dot(a, b):
    return jnp.dot(a, b, preferred_element_type=F32)


def cost(flops, nbytes):
    return pl.CostEstimate(flops=int(flops), bytes_accessed=int(nbytes), transcendentals=0)


def shared_body(x_ref, g_ref, u_ref, d_ref, y_ref, *, rows):
    step = pl.program_id(0)
    tokens, width = x_ref.shape[0], g_ref.shape[1]
    depth = d_ref.shape[1]

    def one(i, _):
        r = pl.ds(pl.multiple_of(i * rows, rows), rows)
        x = x_ref[r, :]
        hs = []
        for c in range(0, width, 256):
            g = dot(x, g_ref[:, c : c + 256])
            u = dot(x, u_ref[:, c : c + 256])
            hs.append((jax.nn.silu(g) * u).astype(BF16))
        h = jnp.concatenate(hs, axis=1)
        for c in range(0, depth, 256):
            part = dot(h, d_ref[:, c : c + 256])
            prev = y_ref[r, c : c + 256]
            y_ref[r, c : c + 256] = jnp.where(step == 0, part, prev + part)
        return _

    lax.fori_loop(0, tokens // rows, one, 0)


def shared_expert(x, s_gate, s_up, s_down, chunk=512, rows=256):
    tokens, d = x.shape
    f = s_gate.shape[1]
    return pl.pallas_call(
        functools.partial(shared_body, rows=rows),
        grid=(f // chunk,),
        in_specs=[
            pl.BlockSpec((tokens, d), lambda i: (0, 0)),
            pl.BlockSpec((d, chunk), lambda i: (0, i)),
            pl.BlockSpec((d, chunk), lambda i: (0, i)),
            pl.BlockSpec((chunk, d), lambda i: (i, 0)),
        ],
        out_specs=pl.BlockSpec((tokens, d), lambda i: (0, 0)),
        out_shape=jax.ShapeDtypeStruct((tokens, d), F32),
        compiler_params=pltpu.CompilerParams(vmem_limit_bytes=56 * MIB),
        cost_estimate=cost(6 * tokens * d * f, 3 * d * f * 2),
        name="shared",
    )(x, s_gate, s_up, s_down)


def dispatch_body(nblk_ref, pos_ref, x_ref, z_ref):
    b = pl.program_id(0)

    @pl.when(b < nblk_ref[0])
    def _():
        tokens = x_ref.shape[0]
        row = b * BLK + lax.broadcasted_iota(jnp.int32, (BLK, tokens), 0)
        hit = pos_ref[0:1, :] == row
        for j in range(1, pos_ref.shape[0]):
            hit = hit | (pos_ref[j : j + 1, :] == row)
        p = jnp.where(hit, 1.0, 0.0).astype(BF16)
        for c in range(0, x_ref.shape[1], 256):
            z_ref[:, c : c + 256] = dot(p, x_ref[:, c : c + 256]).astype(BF16)


def dispatch(nblk, pos, x, rows):
    tokens, d = x.shape
    last = lambda b, n: jnp.minimum(b, jnp.maximum(n[0] - 1, 0))
    return pl.pallas_call(
        dispatch_body,
        grid_spec=pltpu.PrefetchScalarGridSpec(
            num_scalar_prefetch=1,
            grid=(rows // BLK,),
            in_specs=[
                pl.BlockSpec(pos.shape, lambda b, n: (0, 0)),
                pl.BlockSpec((tokens, d), lambda b, n: (0, 0)),
            ],
            out_specs=pl.BlockSpec((BLK, d), lambda b, n: (last(b, n), 0)),
        ),
        out_shape=jax.ShapeDtypeStruct((rows, d), BF16),
        compiler_params=pltpu.CompilerParams(vmem_limit_bytes=32 * MIB),
        cost_estimate=cost(2 * tokens * d * rows // 3, 8 * MIB),
        name="dispatch",
    )(nblk, pos, x)


def rows_of(n_ref, e, sources, experts):
    total = 0
    for q in range(sources):
        total = total + n_ref[q * experts + e]
    return total


def gate_up_body(n_ref, off_ref, wg_ref, wu_ref, *rest, experts, sources):
    z_refs, h_ref, zs, sem = rest[:sources], rest[sources], rest[sources + 1], rest[sources + 2]
    e = pl.program_id(0)
    width = wg_ref.shape[1]

    def fetch(e, slot):
        at = 0
        for q in range(sources):
            n = n_ref[q * experts + e]
            off = off_ref[q * experts + e]

            def one(i, _):
                src = pl.ds(pl.multiple_of(off + i * ROW, ROW), ROW)
                dst = pl.ds(pl.multiple_of(at + i * ROW, ROW), ROW)
                pltpu.make_async_copy(z_refs[q].at[src, :], zs.at[slot, dst, :], sem.at[slot]).start()
                return _

            lax.fori_loop(0, n // ROW, one, 0)
            at = at + n

    @pl.when(e == 0)
    def _():
        fetch(0, 0)

    @pl.when(e + 1 < experts)
    def _():
        fetch(e + 1, (e + 1) % 2)

    slot = e % 2
    total = rows_of(n_ref, e, sources, experts)

    def wait(i, _):
        r = pl.ds(0, ROW)
        pltpu.make_async_copy(z_refs[0].at[r, :], zs.at[slot, r, :], sem.at[slot]).wait()
        return _

    lax.fori_loop(0, total // ROW, wait, 0)

    def block(b, _):
        r = pl.ds(pl.multiple_of(b * BLK, BLK), BLK)
        z = zs[slot, r, :]
        whole = width // 256 * 256
        for c in range(0, whole, 256):
            g = dot(z, wg_ref[:, c : c + 256])
            u = dot(z, wu_ref[:, c : c + 256])
            h_ref[r, c : c + 256] = (jax.nn.silu(g) * u).astype(BF16)
        if whole < width:
            left = width - whole
            gu = dot(z, jnp.concatenate([wg_ref[:, whole:], wu_ref[:, whole:]], axis=1))
            h_ref[r, whole:] = (jax.nn.silu(gu[:, :left]) * gu[:, left:]).astype(BF16)
        return _

    lax.fori_loop(0, pl.cdiv(total, BLK), block, 0)


def gate_up(n, off, w_gate, w_up, zs, most):
    experts, d, f = w_gate.shape
    sources = len(zs)
    return pl.pallas_call(
        functools.partial(gate_up_body, experts=experts, sources=sources),
        grid_spec=pltpu.PrefetchScalarGridSpec(
            num_scalar_prefetch=2,
            grid=(experts,),
            in_specs=[
                pl.BlockSpec((None, d, f), lambda e, *_: (e, 0, 0)),
                pl.BlockSpec((None, d, f), lambda e, *_: (e, 0, 0)),
            ]
            + [pl.BlockSpec(memory_space=pl.ANY)] * sources,
            out_specs=pl.BlockSpec((None, most, f), lambda e, *_: (e, 0, 0)),
            scratch_shapes=[
                pltpu.VMEM((2, most, d), BF16),
                pltpu.SemaphoreType.DMA((2,)),
            ],
        ),
        out_shape=jax.ShapeDtypeStruct((experts, most, f), BF16),
        compiler_params=pltpu.CompilerParams(vmem_limit_bytes=56 * MIB),
        cost_estimate=cost(4 * experts * 256 * d * f, 2 * experts * d * f * 2),
        name="gate_up",
    )(n, off, w_gate, w_up, *zs)


def down_body(n_ref, off_ref, k_ref, wd_ref, h_ref, c_ref, *rest, experts, sources):
    y_refs, (hb, stage, outs, cb, sem, csem) = rest[:sources], rest[sources:]
    e = pl.program_id(0)

    def fetch(e, slot):
        total = rows_of(n_ref, e, sources, experts)

        def one(b, _):
            r = pl.ds(pl.multiple_of(b * BLK, BLK), BLK)
            pltpu.make_async_copy(h_ref.at[e, r, :], hb.at[slot, r, :], sem.at[slot]).start()
            return _

        lax.fori_loop(0, pl.cdiv(total, BLK), one, 0)

    def c_copy(q):
        return pltpu.make_async_copy(c_ref.at[q], cb.at[q % 2], csem.at[q % 2])

    @pl.when(e == 0)
    def _():
        fetch(0, 0)
        c_copy(0).start()
        if sources > 1:
            c_copy(1).start()
        outs[...] = jnp.zeros_like(outs)

    @pl.when(e + 1 < experts)
    def _():
        fetch(e + 1, (e + 1) % 2)

    slot = e % 2
    total = rows_of(n_ref, e, sources, experts)
    blocks = pl.cdiv(total, BLK)

    def block(b, _):
        r = pl.ds(pl.multiple_of(b * BLK, BLK), BLK)
        pltpu.make_async_copy(h_ref.at[0, pl.ds(0, BLK), :], hb.at[slot, pl.ds(0, BLK), :], sem.at[slot]).wait()
        return _

    lax.fori_loop(0, blocks, block, 0)

    def compute(b, _):
        r = pl.ds(pl.multiple_of(b * BLK, BLK), BLK)
        h = hb[slot, r, :]
        for c in range(0, wd_ref.shape[1], 256):
            stage[r, c : c + 256] = dot(h, wd_ref[:, c : c + 256]).astype(BF16)
        return _

    lax.fori_loop(0, blocks, compute, 0)

    at = 0
    for q in range(sources):
        n = n_ref[q * experts + e]
        off = off_ref[q * experts + e]

        def move(i, _):
            src = pl.ds(pl.multiple_of(at + i * ROW, ROW), ROW)
            dst = pl.ds(pl.multiple_of(off + i * ROW, ROW), ROW)
            outs[q, dst, :] = stage[src, :]
            return _

        lax.fori_loop(0, n // ROW, move, 0)
        at = at + n

    @pl.when(e == experts - 1)
    def _():
        tokens, columns = y_refs[0].shape
        for q in range(sources):
            c_copy(q).wait()

            def part(k, acc_from):
                r = pl.ds(pl.multiple_of(k * 256, 256), 256)
                for t in range(0, tokens, 256):
                    cm = cb[q % 2, t : t + 256, r]
                    for c in range(0, columns, 256):
                        p = dot(cm, outs[q, r, c : c + 256])
                        acc[t : t + 256, c : c + 256] = jnp.where(k == 0, p, acc[t : t + 256, c : c + 256] + p)
                return acc_from

            acc = y_refs[q]
            lax.fori_loop(0, jnp.maximum(k_ref[q], 1), part, 0)
            if q + 2 < sources:
                c_copy(q + 2).start()


def down(n, off, k, w_down, h, comb, column, columns):
    experts, f, d = w_down.shape
    sources, tokens, rows = comb.shape
    most = h.shape[1]
    return pl.pallas_call(
        functools.partial(down_body, experts=experts, sources=sources),
        grid_spec=pltpu.PrefetchScalarGridSpec(
            num_scalar_prefetch=3,
            grid=(experts,),
            in_specs=[
                pl.BlockSpec((None, f, columns), lambda e, *_: (e, 0, column // columns)),
                pl.BlockSpec(memory_space=pl.ANY),
                pl.BlockSpec(memory_space=pl.ANY),
            ],
            out_specs=[pl.BlockSpec((tokens, columns), lambda e, *_: (0, 0))] * sources,
            scratch_shapes=[
                pltpu.VMEM((2, most, f), BF16),
                pltpu.VMEM((most, columns), BF16),
                pltpu.VMEM((sources, rows, columns), BF16),
                pltpu.VMEM((2, tokens, rows), BF16),
                pltpu.SemaphoreType.DMA((2,)),
                pltpu.SemaphoreType.DMA((2,)),
            ],
        ),
        out_shape=[jax.ShapeDtypeStruct((tokens, columns), F32)] * sources,
        compiler_params=pltpu.CompilerParams(vmem_limit_bytes=56 * MIB),
        cost_estimate=cost(2 * experts * 256 * f * columns, experts * f * columns * 2),
        name="down",
    )(n, off, k, w_down, h, comb)


def layer(x, expert, slot, gate, w_gate, w_up, w_down, s_gate, s_up, s_down, *, members, experts):
    x, expert, slot, gate = x[0, 0], expert[0, 0], slot[0, 0], gate[0, 0]
    tokens, d = x.shape
    local = w_gate.shape[0]
    slots = 5 * tokens * expert.shape[1] // (4 * experts)
    most_q = pl.cdiv(slots, ROW) * ROW
    rows = pl.cdiv(local * most_q, 256) * 256
    most = pl.cdiv(members * most_q, BLK) * BLK
    me = lax.axis_index("ep")

    def swap(v, q):
        return lax.ppermute(v, "ep", [(i, i ^ q) for i in range(members)])

    mark = (expert * 128 + jnp.minimum(slot, 127)).astype(F32)
    meta = jnp.stack([mark.T, gate.T])
    metas = jnp.stack([meta] + [swap(meta, q) for q in range(1, members)])
    far = swap(x, 2)
    near = swap(x, 1)

    mark = metas[:, 0].astype(jnp.int32)
    where, s = (mark >> 7) - me * local, mark & 127
    ok = (where >= 0) & (where < local) & (s < slots)
    ids = jnp.arange(local, dtype=jnp.int32)
    is_it = (where[:, None] == ids[None, :, None, None]) & ok[:, None]
    n = jnp.max(jnp.where(is_it, s[:, None] + 1, 0), axis=(2, 3))
    n = (n + ROW - 1) // ROW * ROW
    off = jnp.sum(jnp.where(ids[None, :] < ids[:, None], n[:, None, :], 0), axis=2)
    used = jnp.sum(n, axis=1)
    pos = jnp.where(ok, jnp.sum(jnp.where(is_it, off[:, :, None, None], 0), axis=1) + s, -1)
    weight = metas[:, 1].astype(BF16)
    at = jnp.arange(rows, dtype=jnp.int32)
    comb = jnp.zeros((members, tokens, rows), BF16)
    for j in range(pos.shape[1]):
        comb = jnp.where(pos[:, j, :, None] == at, weight[:, j, :, None], comb)

    nf, of = n.reshape(-1), off.reshape(-1)
    nblk = (used + BLK - 1) // BLK
    k = (used + 255) // 256
    send = lambda q, v: dispatch(nblk[q : q + 1], pos[q], v, rows)

    y_shared = shared_expert(x, s_gate, s_up, s_down)
    z = [send(0, x), send(1, near)]
    far_near = swap(far, 1)
    z += [send(2, far), send(3, far_near)]
    h = gate_up(nf, of, w_gate, w_up, z, most)

    columns = 512
    out = []
    for c in range(0, d, columns):
        y0, y1, y2, y3 = down(nf, of, k, w_down, h, comb, c, columns)
        mine = y2 + swap(y3.astype(BF16), 1).astype(F32)
        back = swap(mine.astype(BF16), 2).astype(F32)
        side = swap(y1.astype(BF16), 1).astype(F32)
        out.append((y_shared[:, c : c + columns] + y0 + side + back).astype(BF16))
    return jnp.concatenate(out, axis=1)[None, None]


def solution(mesh):
    members = mesh.shape["ep"]
    tok = P("dp", "ep", None, None)
    w = P("ep", None, None)
    rep = P(None, None)

    def step(x, expert, slot, gate, w_gate, w_up, w_down, s_gate, s_up, s_down):
        body = functools.partial(layer, members=members, experts=w_gate.shape[0])
        return jax.shard_map(
            body,
            mesh=mesh,
            in_specs=(tok, tok, tok, tok, w, w, w, rep, rep, rep),
            out_specs=tok,
            check_vma=False,
        )(x, expert, slot, gate, w_gate, w_up, w_down, s_gate, s_up, s_down)

    return step
```

```python
import functools

import jax
import jax.numpy as jnp
from jax import lax
from jax.experimental import pallas as pl
from jax.experimental.pallas import tpu as pltpu
from jax.sharding import PartitionSpec as P


MIB = 1 << 20
ROW = 16
BLK = 128
F32, BF16 = jnp.float32, jnp.bfloat16


def dot(a, b):
    return jnp.dot(a, b, preferred_element_type=F32)


def cost(flops, nbytes):
    return pl.CostEstimate(flops=int(flops), bytes_accessed=int(nbytes), transcendentals=0)


def shared_body(x_ref, g_ref, u_ref, d_ref, *rest, rows):
    init_ref, y_ref = rest if len(rest) == 2 else (None, rest[0])
    step = pl.program_id(0)
    tokens, width = x_ref.shape[0], g_ref.shape[1]
    depth = d_ref.shape[1]

    @pl.when(step == 0)
    def _():
        if init_ref is None:
            y_ref[...] = jnp.zeros_like(y_ref)
        else:
            y_ref[...] = init_ref[...]

    def one(i, _):
        r = pl.ds(pl.multiple_of(i * rows, rows), rows)
        x = x_ref[r, :]
        hs = []
        for c in range(0, width, 256):
            g = dot(x, g_ref[:, c : c + 256])
            u = dot(x, u_ref[:, c : c + 256])
            hs.append((jax.nn.silu(g) * u).astype(BF16))
        h = jnp.concatenate(hs, axis=1)
        for c in range(0, depth, 256):
            y_ref[r, c : c + 256] += dot(h, d_ref[:, c : c + 256])
        return _

    lax.fori_loop(0, tokens // rows, one, 0)


def shared_expert(x, s_gate, s_up, s_down, first, last, init=None, chunk=512, rows=256):
    tokens, d = x.shape
    once = dict(pipeline_mode=pl.Buffered(1))
    return pl.pallas_call(
        functools.partial(shared_body, rows=rows),
        grid=(last - first,),
        in_specs=[
            pl.BlockSpec((tokens, d), lambda i: (0, 0), **once),
            pl.BlockSpec((d, chunk), lambda i: (0, i + first)),
            pl.BlockSpec((d, chunk), lambda i: (0, i + first)),
            pl.BlockSpec((chunk, d), lambda i: (i + first, 0)),
        ]
        + ([] if init is None else [pl.BlockSpec((tokens, d), lambda i: (0, 0), **once)]),
        out_specs=pl.BlockSpec((tokens, d), lambda i: (0, 0), **once),
        out_shape=jax.ShapeDtypeStruct((tokens, d), F32),
        compiler_params=pltpu.CompilerParams(vmem_limit_bytes=60 * MIB),
        cost_estimate=cost(6 * tokens * d * chunk * (last - first), 6 * d * chunk * (last - first)),
        name="shared",
    )(x, s_gate, s_up, s_down, *(() if init is None else (init,)))


def dispatch_body(nblk_ref, pos_ref, x_ref, z_ref):
    b = pl.program_id(0)

    @pl.when(b < nblk_ref[0])
    def _():
        tokens = x_ref.shape[0]
        row = b * BLK + lax.broadcasted_iota(jnp.int32, (BLK, tokens), 0)
        hit = pos_ref[0:1, :] == row
        for j in range(1, pos_ref.shape[0]):
            hit = hit | (pos_ref[j : j + 1, :] == row)
        p = jnp.where(hit, 1.0, 0.0).astype(BF16)
        for c in range(0, x_ref.shape[1], 256):
            z_ref[:, c : c + 256] = dot(p, x_ref[:, c : c + 256]).astype(BF16)


def dispatch(nblk, pos, x, rows):
    tokens, d = x.shape
    last = lambda b, n: jnp.minimum(b, jnp.maximum(n[0] - 1, 0))
    return pl.pallas_call(
        dispatch_body,
        grid_spec=pltpu.PrefetchScalarGridSpec(
            num_scalar_prefetch=1,
            grid=(rows // BLK,),
            in_specs=[
                pl.BlockSpec(pos.shape, lambda b, n: (0, 0)),
                pl.BlockSpec((tokens, d), lambda b, n: (0, 0)),
            ],
            out_specs=pl.BlockSpec((BLK, d), lambda b, n: (last(b, n), 0)),
        ),
        out_shape=jax.ShapeDtypeStruct((rows, d), BF16),
        compiler_params=pltpu.CompilerParams(vmem_limit_bytes=60 * MIB),
        cost_estimate=cost(2 * tokens * d * rows // 3, 8 * MIB),
        name="dispatch",
    )(nblk, pos, x)


def rows_of(n_ref, e, sources, experts):
    total = 0
    for q in range(sources):
        total = total + n_ref[q * experts + e]
    return total


def gate_up_body(n_ref, off_ref, wg_ref, wu_ref, *rest, experts, sources):
    z_refs, h_ref, zs, sem = rest[:sources], rest[sources], rest[sources + 1], rest[sources + 2]
    e = pl.program_id(0)
    width = wg_ref.shape[1]

    def fetch(e, slot):
        at = 0
        for q in range(sources):
            n = n_ref[q * experts + e]
            off = off_ref[q * experts + e]

            def one(i, _):
                src = pl.ds(pl.multiple_of(off + i * ROW, ROW), ROW)
                dst = pl.ds(pl.multiple_of(at + i * ROW, ROW), ROW)
                pltpu.make_async_copy(z_refs[q].at[src, :], zs.at[slot, dst, :], sem.at[slot]).start()
                return _

            lax.fori_loop(0, n // ROW, one, 0)
            at = at + n

    @pl.when(e == 0)
    def _():
        fetch(0, 0)

    @pl.when(e + 1 < experts)
    def _():
        fetch(e + 1, (e + 1) % 2)

    slot = e % 2
    total = rows_of(n_ref, e, sources, experts)

    def wait(i, _):
        r = pl.ds(0, ROW)
        pltpu.make_async_copy(z_refs[0].at[r, :], zs.at[slot, r, :], sem.at[slot]).wait()
        return _

    lax.fori_loop(0, total // ROW, wait, 0)

    def block(rows):
        z = zs[slot, :rows, :]
        whole = width // 256 * 256
        for c in range(0, whole, 256):
            g = dot(z, wg_ref[:, c : c + 256])
            u = dot(z, wu_ref[:, c : c + 256])
            h_ref[:rows, c : c + 256] = (jax.nn.silu(g) * u).astype(BF16)
        if whole < width:
            left = width - whole
            gu = dot(z, jnp.concatenate([wg_ref[:, whole:], wu_ref[:, whole:]], axis=1))
            h_ref[:rows, whole:] = (jax.nn.silu(gu[:, :left]) * gu[:, left:]).astype(BF16)

    for rows in range(BLK, zs.shape[1] + 1, BLK):
        pl.when((total > rows - BLK) & (total <= rows))(functools.partial(block, rows))


def gate_up(n, off, w_gate, w_up, zs, most):
    experts, d, f = w_gate.shape
    sources = len(zs)
    return pl.pallas_call(
        functools.partial(gate_up_body, experts=experts, sources=sources),
        grid_spec=pltpu.PrefetchScalarGridSpec(
            num_scalar_prefetch=2,
            grid=(experts,),
            in_specs=[
                pl.BlockSpec((None, d, f), lambda e, *_: (e, 0, 0)),
                pl.BlockSpec((None, d, f), lambda e, *_: (e, 0, 0)),
            ]
            + [pl.BlockSpec(memory_space=pl.ANY)] * sources,
            out_specs=pl.BlockSpec((None, most, f), lambda e, *_: (e, 0, 0)),
            scratch_shapes=[
                pltpu.VMEM((2, most, d), BF16),
                pltpu.SemaphoreType.DMA((2,)),
            ],
        ),
        out_shape=jax.ShapeDtypeStruct((experts, most, f), BF16),
        compiler_params=pltpu.CompilerParams(vmem_limit_bytes=60 * MIB),
        cost_estimate=cost(4 * experts * 256 * d * f, 2 * experts * d * f * 2),
        name="gate_up",
    )(n, off, w_gate, w_up, *zs)


def down_body(n_ref, off_ref, k_ref, wd_ref, h_ref, c_ref, *rest, experts, sources, group):
    y_refs, (hb, stage, outs, cb, acc, sem, csem) = rest[:sources], rest[sources:]
    step = pl.program_id(0)

    def c_copy(q):
        return pltpu.make_async_copy(c_ref.at[q], cb.at[q % 2], csem.at[q % 2])

    def h_copy(e, b):
        r = pl.ds(pl.multiple_of(b * BLK, BLK), BLK)
        return pltpu.make_async_copy(h_ref.at[e, r, :], hb.at[e, r, :], sem.at[e])

    @pl.when(step == 0)
    def _():
        def fetch(e, _):
            def one(b, _):
                h_copy(e, b).start()
                return _

            lax.fori_loop(0, pl.cdiv(rows_of(n_ref, e, sources, experts), BLK), one, 0)
            return _

        lax.fori_loop(0, experts, fetch, 0)
        for q in range(2):
            c_copy(sources - 1 - q).start()
        outs[...] = jnp.zeros_like(outs)

    def expert(g, _):
        e = step * group + g
        total = rows_of(n_ref, e, sources, experts)
        blocks = pl.cdiv(total, BLK)

        def arrive(b, _):
            h_copy(e, b).wait()
            return _

        lax.fori_loop(0, blocks, arrive, 0)

        def compute(b, _):
            r = pl.ds(pl.multiple_of(b * BLK, BLK), BLK)
            h = hb[e, r, :]
            for c in range(0, wd_ref.shape[2], 256):
                stage[r, c : c + 256] = dot(h, wd_ref[g, :, c : c + 256]).astype(BF16)
            return _

        lax.fori_loop(0, blocks, compute, 0)

        at = 0
        for q in range(sources):
            n = n_ref[q * experts + e]
            off = off_ref[q * experts + e]

            def move(i, _):
                src = pl.ds(pl.multiple_of(at + i * ROW, ROW), ROW)
                dst = pl.ds(pl.multiple_of(off + i * ROW, ROW), ROW)
                outs[q, dst, :] = stage[src, :]
                return _

            lax.fori_loop(0, n // ROW, move, 0)
            at = at + n
        return _

    lax.fori_loop(0, group, expert, 0)

    @pl.when(step == experts // group - 1)
    def _():
        tokens, columns = acc.shape
        for q in reversed(range(sources)):
            c_copy(q).wait()
            acc[...] = jnp.zeros_like(acc)

            def part(k, _):
                r = pl.ds(pl.multiple_of(k * 256, 256), 256)
                for t in range(0, tokens, 256):
                    cm = cb[q % 2, t : t + 256, r]
                    for c in range(0, columns, 256):
                        acc[t : t + 256, c : c + 256] += dot(cm, outs[q, r, c : c + 256])
                return _

            lax.fori_loop(0, k_ref[q], part, 0)
            y_refs[q][...] = acc[...].astype(y_refs[q].dtype)
            if q >= 2:
                c_copy(q - 2).start()


def down(n, off, k, w_down, h, comb, column, columns, group=3):
    experts, f, d = w_down.shape
    sources, tokens, rows = comb.shape
    most = h.shape[1]
    once = dict(pipeline_mode=pl.Buffered(1))
    return pl.pallas_call(
        functools.partial(down_body, experts=experts, sources=sources, group=group),
        grid_spec=pltpu.PrefetchScalarGridSpec(
            num_scalar_prefetch=3,
            grid=(experts // group,),
            in_specs=[
                pl.BlockSpec((group, f, columns), lambda e, *_: (e, 0, column // columns)),
                pl.BlockSpec(memory_space=pl.ANY),
                pl.BlockSpec(memory_space=pl.ANY),
            ],
            out_specs=[pl.BlockSpec((tokens, columns), lambda e, *_: (0, 0), **once)] * sources,
            scratch_shapes=[
                pltpu.VMEM((experts, most, f), BF16),
                pltpu.VMEM((most, columns), BF16),
                pltpu.VMEM((sources, rows, columns), BF16),
                pltpu.VMEM((2, tokens, rows), BF16),
                pltpu.VMEM((tokens, columns), F32),
                pltpu.SemaphoreType.DMA((experts,)),
                pltpu.SemaphoreType.DMA((2,)),
            ],
        ),
        out_shape=[jax.ShapeDtypeStruct((tokens, columns), F32 if q % 2 == 0 else BF16) for q in range(sources)],
        compiler_params=pltpu.CompilerParams(vmem_limit_bytes=60 * MIB),
        cost_estimate=cost(2 * experts * 256 * f * columns, experts * f * columns * 2),
        name="down",
    )(n, off, k, w_down, h, comb)


def layer(x, expert, slot, gate, w_gate, w_up, w_down, s_gate, s_up, s_down, *, members, experts):
    x, expert, slot, gate = x[0, 0], expert[0, 0], slot[0, 0], gate[0, 0]
    tokens, d = x.shape
    local = w_gate.shape[0]
    slots = 5 * tokens * expert.shape[1] // (4 * experts)
    most_q = pl.cdiv(slots, ROW) * ROW
    rows = pl.cdiv(local * most_q, 256) * 256
    most = pl.cdiv(members * most_q, BLK) * BLK
    me = lax.axis_index("ep")

    def swap(v, q):
        return lax.ppermute(v, "ep", [(i, i ^ q) for i in range(members)])

    mark = (expert * 128 + jnp.minimum(slot, 127)).astype(F32)
    meta = jnp.stack([mark.T, gate.T])
    metas = [meta]
    for q in range(1, members):
        metas.append(swap(meta, q))
    metas = jnp.stack(metas)
    far = swap(x, 2)
    near = swap(x, 1)

    mark = metas[:, 0].astype(jnp.int32)
    where, s = (mark >> 7) - me * local, mark & 127
    ok = (where >= 0) & (where < local) & (s < slots)
    ids = jnp.arange(local, dtype=jnp.int32)
    is_it = (where[:, None] == ids[None, :, None, None]) & ok[:, None]
    n = jnp.max(jnp.where(is_it, s[:, None] + 1, 0), axis=(2, 3))
    n = (n + ROW - 1) // ROW * ROW
    off = jnp.sum(jnp.where(ids[None, :] < ids[:, None], n[:, None, :], 0), axis=2)
    used = jnp.sum(n, axis=1)
    pos = jnp.where(ok, jnp.sum(jnp.where(is_it, off[:, :, None, None], 0), axis=1) + s, -1)
    weight = metas[:, 1].astype(BF16)
    at = jnp.arange(rows, dtype=jnp.int32)
    comb = jnp.zeros((members, tokens, rows), BF16)
    for j in range(pos.shape[1]):
        comb = jnp.where(pos[:, j, :, None] == at, weight[:, j, :, None], comb)

    nf, of = n.reshape(-1), off.reshape(-1)
    nblk = (used + BLK - 1) // BLK
    k = (used + 255) // 256

    def send(q, v):
        return dispatch(nblk[q : q + 1], pos[q], v, rows)

    chunks = s_gate.shape[1] // 512
    cut = chunks * 2 // 3
    y_shared = shared_expert(x, s_gate, s_up, s_down, 0, cut)
    z = [send(0, x), send(1, near)]
    far_near = swap(far, 1)
    z += [send(2, far), send(3, far_near)]
    h = gate_up(nf, of, w_gate, w_up, z, most)

    columns = 512
    own, side, back = [], [], []
    for c in range(0, d, columns):
        y0, y1, y2, y3 = down(nf, of, k, w_down, h, comb, c, columns)
        mine = y2 + swap(y3, 1).astype(F32)
        back.append(swap(mine.astype(BF16), 2))
        side.append(swap(y1, 1))
        own.append(y0)
    y_shared = shared_expert(x, s_gate, s_up, s_down, cut, chunks, y_shared)
    out = [
        (y_shared[:, i * columns : (i + 1) * columns] + own[i] + side[i].astype(F32) + back[i].astype(F32)).astype(BF16)
        for i in range(len(own))
    ]
    return jnp.concatenate(out, axis=1)[None, None]


def solution(mesh):
    members = mesh.shape["ep"]
    tok = P("dp", "ep", None, None)
    w = P("ep", None, None)
    rep = P(None, None)

    def step(x, expert, slot, gate, w_gate, w_up, w_down, s_gate, s_up, s_down):
        body = functools.partial(layer, members=members, experts=w_gate.shape[0])
        return jax.shard_map(
            body,
            mesh=mesh,
            in_specs=(tok, tok, tok, tok, w, w, w, rep, rep, rep),
            out_specs=tok,
            check_vma=False,
        )(x, expert, slot, gate, w_gate, w_up, w_down, s_gate, s_up, s_down)

    return step
```

```python
import functools

import jax
import jax.numpy as jnp
from jax import lax
from jax.experimental import pallas as pl
from jax.experimental.pallas import tpu as pltpu
from jax.sharding import PartitionSpec as P


MIB = 1 << 20
ROW = 16
BLK = 128
F32, BF16 = jnp.float32, jnp.bfloat16


def dot(a, b):
    return jnp.dot(a, b, preferred_element_type=F32)


def cost(flops, nbytes):
    return pl.CostEstimate(flops=int(flops), bytes_accessed=int(nbytes), transcendentals=0)


def shared_body(x_ref, g_ref, u_ref, d_ref, *rest, rows):
    init_ref, y_ref = rest if len(rest) == 2 else (None, rest[0])
    step = pl.program_id(0)
    tokens, width = x_ref.shape[0], g_ref.shape[1]
    depth = d_ref.shape[1]

    @pl.when(step == 0)
    def _():
        if init_ref is None:
            y_ref[...] = jnp.zeros_like(y_ref)
        else:
            y_ref[...] = init_ref[...]

    def one(i, _):
        r = pl.ds(pl.multiple_of(i * rows, rows), rows)
        x = x_ref[r, :]
        hs = []
        for c in range(0, width, 256):
            g = dot(x, g_ref[:, c : c + 256])
            u = dot(x, u_ref[:, c : c + 256])
            hs.append((jax.nn.silu(g) * u).astype(BF16))
        h = jnp.concatenate(hs, axis=1)
        for c in range(0, depth, 256):
            y_ref[r, c : c + 256] += dot(h, d_ref[:, c : c + 256])
        return _

    lax.fori_loop(0, tokens // rows, one, 0)


def shared_expert(x, s_gate, s_up, s_down, first, last, init=None, chunk=512, rows=256):
    tokens, d = x.shape
    once = dict(pipeline_mode=pl.Buffered(1))
    return pl.pallas_call(
        functools.partial(shared_body, rows=rows),
        grid=(last - first,),
        in_specs=[
            pl.BlockSpec((tokens, d), lambda i: (0, 0), **once),
            pl.BlockSpec((d, chunk), lambda i: (0, i + first)),
            pl.BlockSpec((d, chunk), lambda i: (0, i + first)),
            pl.BlockSpec((chunk, d), lambda i: (i + first, 0)),
        ]
        + ([] if init is None else [pl.BlockSpec((tokens, d), lambda i: (0, 0), **once)]),
        out_specs=pl.BlockSpec((tokens, d), lambda i: (0, 0), **once),
        out_shape=jax.ShapeDtypeStruct((tokens, d), F32),
        compiler_params=pltpu.CompilerParams(vmem_limit_bytes=60 * MIB),
        cost_estimate=cost(6 * tokens * d * chunk * (last - first), 6 * d * chunk * (last - first)),
        name="shared",
    )(x, s_gate, s_up, s_down, *(() if init is None else (init,)))


def gather_block(pos_ref, x, z, b, out):
    tokens = x.shape[0]
    row = b * BLK + lax.broadcasted_iota(jnp.int32, (BLK, tokens), 0)
    hit = pos_ref[0:1, :] == row
    for j in range(1, pos_ref.shape[0]):
        hit = hit | (pos_ref[j : j + 1, :] == row)
    p = jnp.where(hit, 1.0, 0.0).astype(BF16)
    for c in range(0, x.shape[1], 256):
        z[out, c : c + 256] = dot(p, x[:, c : c + 256]).astype(BF16)


def dispatch_body(nblk_ref, pos_ref, x_ref, z_ref, *, group):
    step = pl.program_id(0)

    def one(i, _):
        gather_block(pos_ref, x_ref, z_ref, step * group + i, pl.ds(pl.multiple_of(i * BLK, BLK), BLK))
        return _

    lax.fori_loop(0, jnp.clip(nblk_ref[0] - step * group, 0, group), one, 0)


def dispatch(nblk, pos, x, rows, group=4):
    tokens, d = x.shape
    last = lambda b, n: jnp.minimum(b, jnp.maximum(pl.cdiv(n[0], group) - 1, 0))
    return pl.pallas_call(
        functools.partial(dispatch_body, group=group),
        grid_spec=pltpu.PrefetchScalarGridSpec(
            num_scalar_prefetch=1,
            grid=(rows // (BLK * group),),
            in_specs=[
                pl.BlockSpec(pos.shape, lambda b, n: (0, 0)),
                pl.BlockSpec((tokens, d), lambda b, n: (0, 0)),
            ],
            out_specs=pl.BlockSpec((BLK * group, d), lambda b, n: (last(b, n), 0)),
        ),
        out_shape=jax.ShapeDtypeStruct((rows, d), BF16),
        compiler_params=pltpu.CompilerParams(vmem_limit_bytes=60 * MIB),
        cost_estimate=cost(2 * tokens * d * rows // 3, 8 * MIB),
        name="dispatch",
    )(nblk, pos, x)


def rows_of(n_ref, e, sources, experts):
    total = 0
    for q in range(sources):
        total = total + n_ref[q * experts + e]
    return total


def gate_up_body(n_ref, off_ref, nblk_ref, wg_ref, wu_ref, *rest, experts, ready, late, halves):
    sources = ready + late
    pos_refs, rest = rest[:late], rest[late:]
    x_refs, rest = rest[: late * halves], rest[late * halves :]
    z_refs, (h_ref, xv, zv, zs, xsem, zsem) = rest[:ready], rest[ready:]
    e = pl.program_id(0)
    width = wg_ref.shape[1]

    def x_copy(i, j):
        size = x_refs[0].shape[0]
        return pltpu.make_async_copy(x_refs[i * halves + j], xv.at[i, pl.ds(j * size, size), :], xsem.at[i, j])

    def z_copy(q, b):
        r = pl.ds(pl.multiple_of(b * BLK, BLK), BLK)
        return pltpu.make_async_copy(z_refs[q].at[r, :], zv.at[q, r, :], zsem.at[q])

    @pl.when(e == 0)
    def _():
        for i in range(late):
            for j in range(halves):
                x_copy(i, j).start()

        def each(q, act):
            def one(b, _):
                act(z_copy(q, b))
                return _

            lax.fori_loop(0, nblk_ref[q], one, 0)

        for q in range(ready):
            each(q, lambda c: c.start())
        for i in range(late):
            for j in range(halves):
                x_copy(i, j).wait()
            q = ready + i

            def one(b, _):
                gather_block(pos_refs[i], xv.at[i], zv.at[q], b, pl.ds(pl.multiple_of(b * BLK, BLK), BLK))
                return _

            lax.fori_loop(0, nblk_ref[q], one, 0)
        for q in range(ready):
            each(q, lambda c: c.wait())

    at = 0
    for q in range(sources):
        n = n_ref[q * experts + e]
        off = off_ref[q * experts + e]

        def move(i, _):
            src = pl.ds(pl.multiple_of(off + i * ROW, ROW), ROW)
            dst = pl.ds(pl.multiple_of(at + i * ROW, ROW), ROW)
            zs[dst, :] = zv[q, src, :]
            return _

        lax.fori_loop(0, n // ROW, move, 0)
        at = at + n
    total = at

    def block(rows):
        z = zs[:rows, :]
        whole = width // 256 * 256
        for c in range(0, whole, 256):
            g = dot(z, wg_ref[:, c : c + 256])
            u = dot(z, wu_ref[:, c : c + 256])
            h_ref[:rows, c : c + 256] = (jax.nn.silu(g) * u).astype(BF16)
        if whole < width:
            left = width - whole
            gu = dot(z, jnp.concatenate([wg_ref[:, whole:], wu_ref[:, whole:]], axis=1))
            h_ref[:rows, whole:] = (jax.nn.silu(gu[:, :left]) * gu[:, left:]).astype(BF16)

    for rows in range(BLK, zs.shape[0] + 1, BLK):
        pl.when((total > rows - BLK) & (total <= rows))(functools.partial(block, rows))


def gate_up(n, off, nblk, w_gate, w_up, pos, xs, zs, most):
    experts, d, f = w_gate.shape
    ready, late, halves = len(zs), len(xs), len(xs[0])
    rows, tokens = zs[0].shape[0], sum(v.shape[0] for v in xs[0])
    return pl.pallas_call(
        functools.partial(gate_up_body, experts=experts, ready=ready, late=late, halves=halves),
        grid_spec=pltpu.PrefetchScalarGridSpec(
            num_scalar_prefetch=3,
            grid=(experts,),
            in_specs=[
                pl.BlockSpec((None, d, f), lambda e, *_: (e, 0, 0)),
                pl.BlockSpec((None, d, f), lambda e, *_: (e, 0, 0)),
            ]
            + [pl.BlockSpec(p.shape, lambda e, *_: (0, 0)) for p in pos]
            + [pl.BlockSpec(memory_space=pl.ANY)] * (late * halves + ready),
            out_specs=pl.BlockSpec((None, most, f), lambda e, *_: (e, 0, 0)),
            scratch_shapes=[
                pltpu.VMEM((late, tokens, d), BF16),
                pltpu.VMEM((ready + late, rows, d), BF16),
                pltpu.VMEM((most, d), BF16),
                pltpu.SemaphoreType.DMA((late, halves)),
                pltpu.SemaphoreType.DMA((ready,)),
            ],
        ),
        out_shape=jax.ShapeDtypeStruct((experts, most, f), BF16),
        compiler_params=pltpu.CompilerParams(vmem_limit_bytes=67_043_328),
        cost_estimate=cost(4 * experts * 256 * d * f, 2 * experts * d * f * 2),
        name="gate_up",
    )(n, off, nblk, w_gate, w_up, *pos, *[v for x in xs for v in x], *zs)


def down_body(n_ref, off_ref, k_ref, wd_ref, h_ref, c_ref, *rest, experts, sources, group):
    y_refs, (hb, stage, outs, cb, sem, csem) = rest[:sources], rest[sources:]
    step = pl.program_id(0)

    def c_copy(q):
        return pltpu.make_async_copy(c_ref.at[q], cb.at[q % 2], csem.at[q % 2])

    def h_copy(e, b):
        r = pl.ds(pl.multiple_of(b * BLK, BLK), BLK)
        return pltpu.make_async_copy(h_ref.at[e, r, :], hb.at[e, r, :], sem.at[e])

    @pl.when(step == 0)
    def _():
        def fetch(e, _):
            def one(b, _):
                h_copy(e, b).start()
                return _

            lax.fori_loop(0, pl.cdiv(rows_of(n_ref, e, sources, experts), BLK), one, 0)
            return _

        lax.fori_loop(0, experts, fetch, 0)
        for q in range(2):
            c_copy(sources - 1 - q).start()
        outs[...] = jnp.zeros_like(outs)

    def expert(g, _):
        e = step * group + g
        total = rows_of(n_ref, e, sources, experts)
        blocks = pl.cdiv(total, BLK)

        def arrive(b, _):
            h_copy(e, b).wait()
            return _

        lax.fori_loop(0, blocks, arrive, 0)

        def compute(rows):
            stage[:rows, :] = dot(hb[e, :rows, :], wd_ref[g]).astype(BF16)

        for rows in range(BLK, stage.shape[0] + 1, BLK):
            pl.when(blocks == rows // BLK)(functools.partial(compute, rows))

        at = 0
        for q in range(sources):
            n = n_ref[q * experts + e]
            off = off_ref[q * experts + e]

            def move(i, _):
                src = pl.ds(pl.multiple_of(at + i * ROW, ROW), ROW)
                dst = pl.ds(pl.multiple_of(off + i * ROW, ROW), ROW)
                outs[q, dst, :] = stage[src, :]
                return _

            lax.fori_loop(0, n // ROW, move, 0)
            at = at + n
        return _

    lax.fori_loop(0, group, expert, 0)

    @pl.when(step == experts // group - 1)
    def _():
        tokens, columns = y_refs[0].shape
        deepest = outs.shape[1] // 512
        for q in reversed(range(sources)):
            c_copy(q).wait()

            def combine(depth):
                def part(i, _):
                    t = pl.ds(pl.multiple_of(i * 256, 256), 256)
                    y_refs[q][t, :] = dot(cb[q % 2, t, :depth], outs[q, :depth, :]).astype(y_refs[q].dtype)
                    return _

                lax.fori_loop(0, tokens // 256, part, 0)

            for i in range(2, deepest + 1):
                upper = k_ref[q] <= i if i < deepest else True
                lower = k_ref[q] > i - 1 if i > 2 else True
                pl.when(jnp.logical_and(upper, lower))(functools.partial(combine, i * 512))
            if q >= 2:
                c_copy(q - 2).start()


def down(n, off, k, w_down, h, comb, column, columns, group=3):
    experts, f, d = w_down.shape
    sources, tokens, rows = comb.shape
    most = h.shape[1]
    once = dict(pipeline_mode=pl.Buffered(1))
    return pl.pallas_call(
        functools.partial(down_body, experts=experts, sources=sources, group=group),
        grid_spec=pltpu.PrefetchScalarGridSpec(
            num_scalar_prefetch=3,
            grid=(experts // group,),
            in_specs=[
                pl.BlockSpec((group, f, columns), lambda e, *_: (e, 0, column // columns)),
                pl.BlockSpec(memory_space=pl.ANY),
                pl.BlockSpec(memory_space=pl.ANY),
            ],
            out_specs=[pl.BlockSpec((tokens, columns), lambda e, *_: (0, 0), **once)] * sources,
            scratch_shapes=[
                pltpu.VMEM((experts, most, f), BF16),
                pltpu.VMEM((most, columns), BF16),
                pltpu.VMEM((sources, rows, columns), BF16),
                pltpu.VMEM((2, tokens, rows), BF16),
                pltpu.SemaphoreType.DMA((experts,)),
                pltpu.SemaphoreType.DMA((2,)),
            ],
        ),
        out_shape=[jax.ShapeDtypeStruct((tokens, columns), F32 if q % 2 == 0 else BF16) for q in range(sources)],
        compiler_params=pltpu.CompilerParams(vmem_limit_bytes=60 * MIB),
        cost_estimate=cost(2 * experts * 256 * f * columns, experts * f * columns * 2),
        name="down",
    )(n, off, k, w_down, h, comb)


def layer(x, expert, slot, gate, w_gate, w_up, w_down, s_gate, s_up, s_down, *, members, experts):
    x, expert, slot, gate = x[0, 0], expert[0, 0], slot[0, 0], gate[0, 0]
    tokens, d = x.shape
    local = w_gate.shape[0]
    slots = 5 * tokens * expert.shape[1] // (4 * experts)
    most_q = pl.cdiv(slots, ROW) * ROW
    rows = pl.cdiv(local * most_q, 512) * 512
    most = pl.cdiv(members * most_q, BLK) * BLK
    me = lax.axis_index("ep")

    def swap(v, q):
        return lax.ppermute(v, "ep", [(i, i ^ q) for i in range(members)])

    mark = (expert * 128 + jnp.minimum(slot, 127)).astype(F32)
    meta = jnp.stack([mark.T, gate.T])
    metas = [meta]
    for q in range(1, members):
        metas.append(swap(meta, q))
    metas = jnp.stack(metas)
    half = tokens // 2
    far = []
    for i in range(2):
        far.append(swap(x[i * half : (i + 1) * half], 2))
    near = swap(x, 1)

    mark = metas[:, 0].astype(jnp.int32)
    where, s = (mark >> 7) - me * local, mark & 127
    ok = (where >= 0) & (where < local) & (s < slots)
    ids = jnp.arange(local, dtype=jnp.int32)
    is_it = (where[:, None] == ids[None, :, None, None]) & ok[:, None]
    n = jnp.max(jnp.where(is_it, s[:, None] + 1, 0), axis=(2, 3))
    n = (n + ROW - 1) // ROW * ROW
    off = jnp.sum(jnp.where(ids[None, :] < ids[:, None], n[:, None, :], 0), axis=2)
    used = jnp.sum(n, axis=1)
    pos = jnp.where(ok, jnp.sum(jnp.where(is_it, off[:, :, None, None], 0), axis=1) + s, -1)
    weight = metas[:, 1].astype(BF16)
    at = jnp.arange(rows, dtype=jnp.int32)
    comb = jnp.zeros((members, tokens, rows), BF16)
    for j in range(pos.shape[1]):
        comb = jnp.where(pos[:, j, :, None] == at, weight[:, j, :, None], comb)

    nf, of = n.reshape(-1), off.reshape(-1)
    nblk = (used + BLK - 1) // BLK
    k = (used + 511) // 512

    def send(q, v):
        return dispatch(nblk[q : q + 1], pos[q], v, rows)

    chunks = s_gate.shape[1] // 512
    cut = chunks * 2 // 3
    y_shared = shared_expert(x, s_gate, s_up, s_down, 0, cut)
    z = [send(0, x), send(1, near)]
    far_near = []
    for i in range(2):
        far_near.append(swap(far[i], 1))
    h = gate_up(nf, of, nblk, w_gate, w_up, [pos[2], pos[3]], [far, far_near], z, most)

    columns = 512
    own, side, back = [], [], []
    for c in range(0, d, columns):
        y0, y1, y2, y3 = down(nf, of, k, w_down, h, comb, c, columns)
        mine = y2 + swap(y3, 1).astype(F32)
        back.append(swap(mine.astype(BF16), 2))
        side.append(swap(y1, 1))
        own.append(y0)
    y_shared = shared_expert(x, s_gate, s_up, s_down, cut, chunks, y_shared)
    out = [
        (y_shared[:, i * columns : (i + 1) * columns] + own[i] + side[i].astype(F32) + back[i].astype(F32)).astype(BF16)
        for i in range(len(own))
    ]
    return jnp.concatenate(out, axis=1)[None, None]


def solution(mesh):
    members = mesh.shape["ep"]
    tok = P("dp", "ep", None, None)
    w = P("ep", None, None)
    rep = P(None, None)

    def step(x, expert, slot, gate, w_gate, w_up, w_down, s_gate, s_up, s_down):
        body = functools.partial(layer, members=members, experts=w_gate.shape[0])
        return jax.shard_map(
            body,
            mesh=mesh,
            in_specs=(tok, tok, tok, tok, w, w, w, rep, rep, rep),
            out_specs=tok,
            check_vma=False,
        )(x, expert, slot, gate, w_gate, w_up, w_down, s_gate, s_up, s_down)

    return step
```

```python
import functools

import jax
import jax.numpy as jnp
from jax import lax
from jax.experimental import pallas as pl
from jax.experimental.pallas import tpu as pltpu
from jax.sharding import PartitionSpec as P


MIB = 1 << 20
ROW = 16
BLK = 128
DEPTH = 512
F32, BF16 = jnp.float32, jnp.bfloat16


def dot(a, b):
    return jnp.dot(a, b, preferred_element_type=F32)


def cost(flops, nbytes):
    return pl.CostEstimate(flops=int(flops), bytes_accessed=int(nbytes), transcendentals=0)


def shared_body(x_ref, g_ref, u_ref, d_ref, *rest, rows):
    init_ref, y_ref = rest if len(rest) == 2 else (None, rest[0])
    step = pl.program_id(0)
    tokens, width = x_ref.shape[0], g_ref.shape[1]
    depth = d_ref.shape[1]

    @pl.when(step == 0)
    def _():
        if init_ref is None:
            y_ref[...] = jnp.zeros_like(y_ref)
        else:
            y_ref[...] = init_ref[...]

    def one(i, _):
        r = pl.ds(pl.multiple_of(i * rows, rows), rows)
        x = x_ref[r, :]
        hs = []
        for c in range(0, width, 256):
            g = dot(x, g_ref[:, c : c + 256])
            u = dot(x, u_ref[:, c : c + 256])
            hs.append((jax.nn.silu(g) * u).astype(BF16))
        h = jnp.concatenate(hs, axis=1)
        for c in range(0, depth, 256):
            y_ref[r, c : c + 256] += dot(h, d_ref[:, c : c + 256])
        return _

    lax.fori_loop(0, tokens // rows, one, 0)


def shared_expert(x, s_gate, s_up, s_down, first, last, init=None, chunk=512, rows=512):
    tokens, d = x.shape
    once = dict(pipeline_mode=pl.Buffered(1))
    return pl.pallas_call(
        functools.partial(shared_body, rows=rows),
        grid=(last - first,),
        in_specs=[
            pl.BlockSpec((tokens, d), lambda i: (0, 0), **once),
            pl.BlockSpec((d, chunk), lambda i: (0, i + first)),
            pl.BlockSpec((d, chunk), lambda i: (0, i + first)),
            pl.BlockSpec((chunk, d), lambda i: (i + first, 0)),
        ]
        + ([] if init is None else [pl.BlockSpec((tokens, d), lambda i: (0, 0), **once)]),
        out_specs=pl.BlockSpec((tokens, d), lambda i: (0, 0), **once),
        out_shape=jax.ShapeDtypeStruct((tokens, d), F32),
        compiler_params=pltpu.CompilerParams(vmem_limit_bytes=60 * MIB),
        cost_estimate=cost(6 * tokens * d * chunk * (last - first), 6 * d * chunk * (last - first)),
        name="shared",
    )(x, s_gate, s_up, s_down, *(() if init is None else (init,)))


def gather_block(pos_ref, x, z, b, out):
    tokens = x.shape[0]
    row = b * BLK + lax.broadcasted_iota(jnp.int32, (BLK, tokens), 0)
    hit = pos_ref[0:1, :] == row
    for j in range(1, pos_ref.shape[0]):
        hit = hit | (pos_ref[j : j + 1, :] == row)
    p = jnp.where(hit, 1.0, 0.0).astype(BF16)
    for c in range(0, x.shape[1], 256):
        z[out, c : c + 256] = dot(p, x[:, c : c + 256]).astype(BF16)


def dispatch_body(nblk_ref, pos_ref, x_ref, z_ref, *, group):
    step = pl.program_id(0)

    def one(i, _):
        gather_block(pos_ref, x_ref, z_ref, step * group + i, pl.ds(pl.multiple_of(i * BLK, BLK), BLK))
        return _

    lax.fori_loop(0, jnp.clip(nblk_ref[0] - step * group, 0, group), one, 0)


def dispatch(nblk, pos, x, rows, group=4):
    tokens, d = x.shape
    last = lambda b, n: jnp.minimum(b, jnp.maximum(pl.cdiv(n[0], group) - 1, 0))
    return pl.pallas_call(
        functools.partial(dispatch_body, group=group),
        grid_spec=pltpu.PrefetchScalarGridSpec(
            num_scalar_prefetch=1,
            grid=(rows // (BLK * group),),
            in_specs=[
                pl.BlockSpec(pos.shape, lambda b, n: (0, 0)),
                pl.BlockSpec((tokens, d), lambda b, n: (0, 0)),
            ],
            out_specs=pl.BlockSpec((BLK * group, d), lambda b, n: (last(b, n), 0)),
        ),
        out_shape=jax.ShapeDtypeStruct((rows, d), BF16),
        compiler_params=pltpu.CompilerParams(vmem_limit_bytes=60 * MIB),
        cost_estimate=cost(2 * tokens * d * rows // 3, 8 * MIB),
        name="dispatch",
    )(nblk, pos, x)


def rows_of(n_ref, e, sources, experts):
    total = 0
    for q in range(sources):
        total = total + n_ref[q * experts + e]
    return total


def gate_up_body(n_ref, off_ref, nblk_ref, wg_ref, wu_ref, *rest, experts, ready, late, halves):
    sources = ready + late
    pos_refs, rest = rest[:late], rest[late:]
    x_refs, rest = rest[: late * halves], rest[late * halves :]
    z_refs, (h_ref, xv, zv, zs, xsem, zsem) = rest[:ready], rest[ready:]
    e = pl.program_id(0)
    width = wg_ref.shape[1]

    def x_copy(i, j):
        size = x_refs[0].shape[0]
        return pltpu.make_async_copy(x_refs[i * halves + j], xv.at[i, pl.ds(j * size, size), :], xsem.at[i, j])

    def z_copy(q, b):
        r = pl.ds(pl.multiple_of(b * BLK, BLK), BLK)
        return pltpu.make_async_copy(z_refs[q].at[r, :], zv.at[q, r, :], zsem.at[q])

    @pl.when(e == 0)
    def _():
        for i in range(late):
            for j in range(halves):
                x_copy(i, j).start()

        def each(q, act):
            def one(b, _):
                act(z_copy(q, b))
                return _

            lax.fori_loop(0, nblk_ref[q], one, 0)

        for q in range(ready):
            each(q, lambda c: c.start())
        for i in range(late):
            for j in range(halves):
                x_copy(i, j).wait()
            q = ready + i

            def one(b, _):
                gather_block(pos_refs[i], xv.at[i], zv.at[q], b, pl.ds(pl.multiple_of(b * BLK, BLK), BLK))
                return _

            lax.fori_loop(0, nblk_ref[q], one, 0)
        for q in range(ready):
            each(q, lambda c: c.wait())

    at = 0
    for q in range(sources):
        n = n_ref[q * experts + e]
        off = off_ref[q * experts + e]

        def move(i, _):
            src = pl.ds(pl.multiple_of(off + i * ROW, ROW), ROW)
            dst = pl.ds(pl.multiple_of(at + i * ROW, ROW), ROW)
            zs[dst, :] = zv[q, src, :]
            return _

        lax.fori_loop(0, n // ROW, move, 0)
        at = at + n
    total = at

    def block(rows):
        z = zs[:rows, :]
        whole = width // 256 * 256
        for c in range(0, whole, 256):
            g = dot(z, wg_ref[:, c : c + 256])
            u = dot(z, wu_ref[:, c : c + 256])
            h_ref[:rows, c : c + 256] = (jax.nn.silu(g) * u).astype(BF16)
        if whole < width:
            left = width - whole
            gu = dot(z, jnp.concatenate([wg_ref[:, whole:], wu_ref[:, whole:]], axis=1))
            h_ref[:rows, whole:] = (jax.nn.silu(gu[:, :left]) * gu[:, left:]).astype(BF16)

    for rows in range(BLK, zs.shape[0] + 1, BLK):
        pl.when((total > rows - BLK) & (total <= rows))(functools.partial(block, rows))


def gate_up(n, off, nblk, w_gate, w_up, pos, xs, zs, most):
    experts, d, f = w_gate.shape
    ready, late, halves = len(zs), len(xs), len(xs[0])
    rows, tokens = zs[0].shape[0], sum(v.shape[0] for v in xs[0])
    return pl.pallas_call(
        functools.partial(gate_up_body, experts=experts, ready=ready, late=late, halves=halves),
        grid_spec=pltpu.PrefetchScalarGridSpec(
            num_scalar_prefetch=3,
            grid=(experts,),
            in_specs=[
                pl.BlockSpec((None, d, f), lambda e, *_: (e, 0, 0)),
                pl.BlockSpec((None, d, f), lambda e, *_: (e, 0, 0)),
            ]
            + [pl.BlockSpec(p.shape, lambda e, *_: (0, 0)) for p in pos]
            + [pl.BlockSpec(memory_space=pl.ANY)] * (late * halves + ready),
            out_specs=pl.BlockSpec((None, most, f), lambda e, *_: (e, 0, 0)),
            scratch_shapes=[
                pltpu.VMEM((late, tokens, d), BF16),
                pltpu.VMEM((ready + late, rows, d), BF16),
                pltpu.VMEM((most, d), BF16),
                pltpu.SemaphoreType.DMA((late, halves)),
                pltpu.SemaphoreType.DMA((ready,)),
            ],
        ),
        out_shape=jax.ShapeDtypeStruct((experts, most, f), BF16),
        compiler_params=pltpu.CompilerParams(vmem_limit_bytes=67_043_328),
        cost_estimate=cost(4 * experts * 256 * d * f, 2 * experts * d * f * 2),
        name="gate_up",
    )(n, off, nblk, w_gate, w_up, *pos, *[v for x in xs for v in x], *zs)


def comb_body(k_ref, pos_ref, gate_ref, c_ref):
    q, b = pl.program_id(0), pl.program_id(1)
    tokens, width = c_ref.shape

    @pl.when(b < k_ref[q])
    def _():
        column = b * width + lax.broadcasted_iota(jnp.int32, (BLK, width), 1)

        def one(i, _):
            t = pl.ds(pl.multiple_of(i * BLK, BLK), BLK)
            pos, gate = pos_ref[t, :], gate_ref[t, :]
            value = jnp.zeros((BLK, width), F32)
            for j in range(pos.shape[1]):
                value = jnp.where(pos[:, j : j + 1] == column, gate[:, j : j + 1], value)
            c_ref[t, :] = value.astype(BF16)
            return _

        lax.fori_loop(0, tokens // BLK, one, 0)


def combine_matrices(k, pos, gate, rows):
    sources, tokens, top = pos.shape
    return pl.pallas_call(
        comb_body,
        grid_spec=pltpu.PrefetchScalarGridSpec(
            num_scalar_prefetch=1,
            grid=(sources, rows // DEPTH),
            in_specs=[pl.BlockSpec((None, tokens, top), lambda q, b, k: (q, 0, 0))] * 2,
            out_specs=pl.BlockSpec((None, tokens, DEPTH), lambda q, b, k: (q, 0, jnp.minimum(b, k[q] - 1))),
        ),
        out_shape=jax.ShapeDtypeStruct((sources, tokens, rows), BF16),
        compiler_params=pltpu.CompilerParams(vmem_limit_bytes=60 * MIB),
        cost_estimate=cost(4 * MIB, 8 * MIB),
        name="comb",
    )(k, pos, gate)


def combine(k, c, rows, out):
    deepest = rows.shape[0] // DEPTH

    def whole(depth):
        def part(i, _):
            t = pl.ds(pl.multiple_of(i * 256, 256), 256)
            out(t, dot(c[t, :depth], rows[:depth, :]))
            return _

        lax.fori_loop(0, c.shape[0] // 256, part, 0)

    pl.when(k < deepest)(functools.partial(whole, (deepest - 1) * DEPTH))
    pl.when(k >= deepest)(functools.partial(whole, deepest * DEPTH))


def down_body(n_ref, off_ref, k_ref, wd_ref, h_ref, c_ref, *rest, experts, own, far, group):
    y_refs, own_ref, (hb, stage, outs, cb, sem, csem) = rest[-far - 7 : -7], rest[-7], rest[-6:]
    step = pl.program_id(0)
    sources = own + far

    def c_copy(i):
        return pltpu.make_async_copy(c_ref.at[own + i], cb.at[i], csem.at[i])

    def h_copy(e, b):
        r = pl.ds(pl.multiple_of(b * BLK, BLK), BLK)
        return pltpu.make_async_copy(h_ref.at[e, r, :], hb.at[e, r, :], sem.at[e])

    @pl.when(step == 0)
    def _():
        def fetch(e, _):
            def one(b, _):
                h_copy(e, b).start()
                return _

            lax.fori_loop(0, pl.cdiv(rows_of(n_ref, e, sources, experts), BLK), one, 0)
            return _

        lax.fori_loop(0, experts, fetch, 0)
        for i in range(far):
            c_copy(i).start()
        outs[...] = jnp.zeros_like(outs)
        own_ref[...] = jnp.zeros_like(own_ref)

    def expert(g, _):
        e = step * group + g
        total = rows_of(n_ref, e, sources, experts)
        blocks = pl.cdiv(total, BLK)

        def arrive(b, _):
            h_copy(e, b).wait()
            return _

        lax.fori_loop(0, blocks, arrive, 0)

        def compute(rows):
            stage[:rows, :] = dot(hb[e, :rows, :], wd_ref[g]).astype(BF16)

        for rows in range(BLK, stage.shape[0] + 1, BLK):
            pl.when(blocks == rows // BLK)(functools.partial(compute, rows))

        at = 0
        for q in range(sources):
            n = n_ref[q * experts + e]
            off = off_ref[q * experts + e]
            to = own_ref.at[q] if q < own else outs.at[q - own]

            def move(i, _):
                src = pl.ds(pl.multiple_of(at + i * ROW, ROW), ROW)
                dst = pl.ds(pl.multiple_of(off + i * ROW, ROW), ROW)
                to[dst, :] = stage[src, :]
                return _

            lax.fori_loop(0, n // ROW, move, 0)
            at = at + n
        return _

    lax.fori_loop(0, group, expert, 0)

    @pl.when(step == experts // group - 1)
    def _():
        for i in reversed(range(far)):
            c_copy(i).wait()

            def out(t, v):
                y_refs[i][t, :] = v.astype(y_refs[i].dtype)

            combine(k_ref[own + i], cb.at[i], outs.at[i], out)


def down(n, off, k, w_down, h, comb, kept, column, columns, own, group=3):
    experts, f, d = w_down.shape
    sources, tokens, rows = comb.shape
    far = sources - own
    most = h.shape[1]
    once = dict(pipeline_mode=pl.Buffered(1))
    at = column // columns
    aliased = [] if kept is None else [kept]
    return pl.pallas_call(
        functools.partial(down_body, experts=experts, own=own, far=far, group=group),
        grid_spec=pltpu.PrefetchScalarGridSpec(
            num_scalar_prefetch=3,
            grid=(experts // group,),
            in_specs=[pl.BlockSpec((group, f, columns), lambda e, *_: (e, 0, at))]
            + [pl.BlockSpec(memory_space=pl.ANY)] * (2 + len(aliased)),
            out_specs=[pl.BlockSpec((tokens, columns), lambda e, *_: (0, 0), **once)] * far
            + [pl.BlockSpec((own, rows, columns), lambda e, *_: (0, 0, at), **once)],
            scratch_shapes=[
                pltpu.VMEM((experts, most, f), BF16),
                pltpu.VMEM((most, columns), BF16),
                pltpu.VMEM((far, rows, columns), BF16),
                pltpu.VMEM((far, tokens, rows), BF16),
                pltpu.SemaphoreType.DMA((experts,)),
                pltpu.SemaphoreType.DMA((far,)),
            ],
        ),
        out_shape=[jax.ShapeDtypeStruct((tokens, columns), F32 if i == 0 else BF16) for i in range(far)]
        + [jax.ShapeDtypeStruct((own, rows, d), BF16)],
        input_output_aliases={6: far} if aliased else {},
        compiler_params=pltpu.CompilerParams(vmem_limit_bytes=67_043_328),
        cost_estimate=cost(2 * experts * 256 * f * columns, experts * f * columns * 2),
        name="down",
    )(n, off, k, w_down, h, comb, *aliased)


def own_body(k_ref, c_ref, r_ref, s_ref, *y_refs):
    for i in reversed(range(len(y_refs))):

        def out(t, v):
            y_refs[i][t, :] = v + s_ref[t, :] if i == 0 else v.astype(BF16)

        combine(k_ref[i], c_ref.at[i], r_ref.at[i], out)


def own_sums(k, comb, kept, shared, columns=512):
    own, rows, d = kept.shape
    tokens = comb.shape[1]
    return pl.pallas_call(
        own_body,
        grid_spec=pltpu.PrefetchScalarGridSpec(
            num_scalar_prefetch=1,
            grid=(d // columns,),
            in_specs=[
                pl.BlockSpec((own, tokens, rows), lambda c, *_: (0, 0, 0), pipeline_mode=pl.Buffered(1)),
                pl.BlockSpec((own, rows, columns), lambda c, *_: (0, 0, c)),
                pl.BlockSpec((tokens, columns), lambda c, *_: (0, c)),
            ],
            out_specs=[pl.BlockSpec((tokens, columns), lambda c, *_: (0, c))] * own,
        ),
        out_shape=[jax.ShapeDtypeStruct((tokens, d), F32 if i == 0 else BF16) for i in range(own)],
        compiler_params=pltpu.CompilerParams(vmem_limit_bytes=60 * MIB),
        cost_estimate=cost(4 * tokens * rows * d, 20 * MIB),
        name="own",
    )(k, comb, kept, shared)


def layer(x, expert, slot, gate, w_gate, w_up, w_down, s_gate, s_up, s_down, *, members, experts):
    x, expert, slot, gate = x[0, 0], expert[0, 0], slot[0, 0], gate[0, 0]
    tokens, d = x.shape
    local = w_gate.shape[0]
    slots = 5 * tokens * expert.shape[1] // (4 * experts)
    most_q = pl.cdiv(slots, ROW) * ROW
    rows = pl.cdiv(local * most_q, DEPTH) * DEPTH
    most = pl.cdiv(members * most_q, BLK) * BLK
    me = lax.axis_index("ep")

    def swap(v, q):
        return lax.ppermute(v, "ep", [(i, i ^ q) for i in range(members)])

    mark = (expert * 128 + jnp.minimum(slot, 127)).astype(F32)
    meta = jnp.stack([mark.T, gate.T])
    metas = [meta]
    for q in range(1, members):
        metas.append(swap(meta, q))
    metas = jnp.stack(metas)
    far = swap(x, 2)
    near = swap(x, 1)

    mark = metas[:, 0].astype(jnp.int32)
    where, s = (mark >> 7) - me * local, mark & 127
    ok = (where >= 0) & (where < local) & (s < slots)
    ids = jnp.arange(local, dtype=jnp.int32)
    is_it = (where[:, None] == ids[None, :, None, None]) & ok[:, None]
    n = jnp.max(jnp.where(is_it, s[:, None] + 1, 0), axis=(2, 3))
    n = (n + ROW - 1) // ROW * ROW
    off = jnp.sum(jnp.where(ids[None, :] < ids[:, None], n[:, None, :], 0), axis=2)
    used = jnp.sum(n, axis=1)
    pos = jnp.where(ok, jnp.sum(jnp.where(is_it, off[:, :, None, None], 0), axis=1) + s, -1)
    nf, of = n.reshape(-1), off.reshape(-1)
    nblk = (used + BLK - 1) // BLK
    k = jnp.maximum((used + DEPTH - 1) // DEPTH, rows // DEPTH - 1)

    def send(q, v):
        return dispatch(nblk[q : q + 1], pos[q], v, rows)

    chunks = s_gate.shape[1] // 512
    cut = chunks * 8 // 11
    y_shared = shared_expert(x, s_gate, s_up, s_down, 0, cut)
    z = [send(0, x), send(1, near)]
    far_near = swap(far, 1)
    gates = metas[:, 1].astype(BF16).astype(F32)
    comb = combine_matrices(k, pos.transpose(0, 2, 1), gates.transpose(0, 2, 1), rows)
    h = gate_up(nf, of, nblk, w_gate, w_up, [pos[2], pos[3]], [[far], [far_near]], z, most)

    back, kept, at = [], None, 0
    for columns in (d // 4, d // 4, d // 2):
        y2, y3, kept = down(nf, of, k, w_down, h, comb, kept, at, columns, 2)
        mine = y2 + swap(y3, 1).astype(F32)
        back.append(swap(mine.astype(BF16), 2))
        at += columns
    y0, y1 = own_sums(k, comb, kept, y_shared)
    side = swap(y1, 1)
    y_shared = shared_expert(x, s_gate, s_up, s_down, cut, chunks, y0)
    return (y_shared + side.astype(F32) + jnp.concatenate(back, axis=1).astype(F32)).astype(BF16)[None, None]


def solution(mesh):
    members = mesh.shape["ep"]
    tok = P("dp", "ep", None, None)
    w = P("ep", None, None)
    rep = P(None, None)

    def step(x, expert, slot, gate, w_gate, w_up, w_down, s_gate, s_up, s_down):
        body = functools.partial(layer, members=members, experts=w_gate.shape[0])
        return jax.shard_map(
            body,
            mesh=mesh,
            in_specs=(tok, tok, tok, tok, w, w, w, rep, rep, rep),
            out_specs=tok,
            check_vma=False,
        )(x, expert, slot, gate, w_gate, w_up, w_down, s_gate, s_up, s_down)

    return step
```

```python
import functools

import jax
import jax.numpy as jnp
from jax import lax
from jax.experimental import pallas as pl
from jax.experimental.pallas import tpu as pltpu
from jax.sharding import PartitionSpec as P


MIB = 1 << 20
ROW = 16
BLK = 128
DEPTH = 512
F32, BF16 = jnp.float32, jnp.bfloat16


def dot(a, b):
    return jnp.dot(a, b, preferred_element_type=F32)


def cost(flops, nbytes):
    return pl.CostEstimate(flops=int(flops), bytes_accessed=int(nbytes), transcendentals=0)


def shared_body(x_ref, g_ref, u_ref, d_ref, *rest, rows):
    init_ref, y_ref = rest if len(rest) == 2 else (None, rest[0])
    step = pl.program_id(0)
    tokens, width = x_ref.shape[0], g_ref.shape[1]
    depth = d_ref.shape[1]

    @pl.when(step == 0)
    def _():
        if init_ref is None:
            y_ref[...] = jnp.zeros_like(y_ref)
        else:
            y_ref[...] = init_ref[...]

    def one(i, _):
        r = pl.ds(pl.multiple_of(i * rows, rows), rows)
        x = x_ref[r, :]
        hs = []
        for c in range(0, width, 256):
            g = dot(x, g_ref[:, c : c + 256])
            u = dot(x, u_ref[:, c : c + 256])
            hs.append((jax.nn.silu(g) * u).astype(BF16))
        h = jnp.concatenate(hs, axis=1)
        for c in range(0, depth, 256):
            y_ref[r, c : c + 256] += dot(h, d_ref[:, c : c + 256])
        return _

    lax.fori_loop(0, tokens // rows, one, 0)


def shared_expert(x, s_gate, s_up, s_down, first, last, init=None, chunk=512, rows=512):
    tokens, d = x.shape
    once = dict(pipeline_mode=pl.Buffered(1))
    return pl.pallas_call(
        functools.partial(shared_body, rows=rows),
        grid=(last - first,),
        in_specs=[
            pl.BlockSpec((tokens, d), lambda i: (0, 0), **once),
            pl.BlockSpec((d, chunk), lambda i: (0, i + first)),
            pl.BlockSpec((d, chunk), lambda i: (0, i + first)),
            pl.BlockSpec((chunk, d), lambda i: (i + first, 0)),
        ]
        + ([] if init is None else [pl.BlockSpec((tokens, d), lambda i: (0, 0), **once)]),
        out_specs=pl.BlockSpec((tokens, d), lambda i: (0, 0), **once),
        out_shape=jax.ShapeDtypeStruct((tokens, d), F32),
        compiler_params=pltpu.CompilerParams(vmem_limit_bytes=60 * MIB),
        cost_estimate=cost(6 * tokens * d * chunk * (last - first), 6 * d * chunk * (last - first)),
        name="shared",
    )(x, s_gate, s_up, s_down, *(() if init is None else (init,)))


def picked(values, tokens, first, pos, other=None):
    row = (first + lax.broadcasted_iota(jnp.int32, (values.shape[0], 1), 0)).astype(F32)
    tile = jnp.zeros(values.shape, F32)
    for j in range(pos.shape[0]):
        hit = jnp.broadcast_to(pos[j : j + 1, tokens], values.shape) == row
        tile = jnp.where(hit, 1.0 if other is None else other[j : j + 1, tokens], tile)
    return tile.astype(BF16)


def select_rows(pos, first, out):
    for r in range(0, out.shape[0], 32):
        for t in range(0, out.shape[1], 256):
            tile = out.at[r : r + 32, t : t + 256]
            tile[...] = picked(tile, slice(t, t + 256), first + r, pos)


def gather(count, pos, x, z, p, first=0):
    def one(i, _):
        select_rows(pos, (first + i + 1) * BLK, p.at[(i + 1) % 2])
        r = pl.ds(pl.multiple_of(i * BLK, BLK), BLK)
        for c in range(0, x.shape[1], 256):
            z[r, c : c + 256] = dot(p[i % 2], x[:, c : c + 256]).astype(BF16)
        return _

    pl.when(count > 0)(lambda: select_rows(pos, first * BLK, p.at[0]))
    lax.fori_loop(0, count, one, 0)


def dispatch_body(nblk_ref, pos_ref, x_ref, z_ref, p, *, group):
    step = pl.program_id(0)
    gather(jnp.clip(nblk_ref[0] - step * group, 0, group), pos_ref, x_ref, z_ref, p, step * group)


def dispatch(nblk, pos, x, rows, group=4):
    tokens, d = x.shape
    last = lambda b, n: jnp.minimum(b, jnp.maximum(pl.cdiv(n[0], group) - 1, 0))
    return pl.pallas_call(
        functools.partial(dispatch_body, group=group),
        grid_spec=pltpu.PrefetchScalarGridSpec(
            num_scalar_prefetch=1,
            grid=(rows // (BLK * group),),
            in_specs=[
                pl.BlockSpec(pos.shape, lambda b, n: (0, 0)),
                pl.BlockSpec((tokens, d), lambda b, n: (0, 0)),
            ],
            out_specs=pl.BlockSpec((BLK * group, d), lambda b, n: (last(b, n), 0)),
            scratch_shapes=[pltpu.VMEM((2, BLK, tokens), BF16)],
        ),
        out_shape=jax.ShapeDtypeStruct((rows, d), BF16),
        compiler_params=pltpu.CompilerParams(vmem_limit_bytes=60 * MIB),
        cost_estimate=cost(2 * tokens * d * rows // 3, 8 * MIB),
        name="dispatch",
    )(nblk, pos, x)


def rows_of(n_ref, e, sources, experts):
    total = 0
    for q in range(sources):
        total = total + n_ref[q * experts + e]
    return total


def gate_up_body(n_ref, off_ref, nblk_ref, wg_ref, wu_ref, *rest, experts, ready, late, halves):
    sources = ready + late
    pos_refs, rest = rest[:late], rest[late:]
    x_refs, rest = rest[: late * halves], rest[late * halves :]
    z_refs, (h_ref, xv, zv, zs, p, xsem, zsem) = rest[:ready], rest[ready:]
    e = pl.program_id(0)
    width = wg_ref.shape[1]

    def x_copy(i, j):
        size = x_refs[0].shape[0]
        return pltpu.make_async_copy(x_refs[i * halves + j], xv.at[i, pl.ds(j * size, size), :], xsem.at[i, j])

    def z_copy(q, b):
        r = pl.ds(pl.multiple_of(b * BLK, BLK), BLK)
        return pltpu.make_async_copy(z_refs[q].at[r, :], zv.at[q, r, :], zsem.at[q])

    @pl.when(e == 0)
    def _():
        for i in range(late):
            for j in range(halves):
                x_copy(i, j).start()

        def each(q, act):
            def one(b, _):
                act(z_copy(q, b))
                return _

            lax.fori_loop(0, nblk_ref[q], one, 0)

        for q in range(ready):
            each(q, lambda c: c.start())
        for i in range(late):
            for j in range(halves):
                x_copy(i, j).wait()
            q = ready + i

            gather(nblk_ref[q], pos_refs[i], xv.at[i], zv.at[q], p)
        for q in range(ready):
            each(q, lambda c: c.wait())

    at = 0
    for q in range(sources):
        n = n_ref[q * experts + e]
        off = off_ref[q * experts + e]

        def move(i, _):
            src = pl.ds(pl.multiple_of(off + i * ROW, ROW), ROW)
            dst = pl.ds(pl.multiple_of(at + i * ROW, ROW), ROW)
            zs[dst, :] = zv[q, src, :]
            return _

        lax.fori_loop(0, n // ROW, move, 0)
        at = at + n
    total = at

    def block(rows):
        z = zs[:rows, :]
        whole = width // 256 * 256
        for c in range(0, whole, 256):
            g = dot(z, wg_ref[:, c : c + 256])
            u = dot(z, wu_ref[:, c : c + 256])
            h_ref[:rows, c : c + 256] = (jax.nn.silu(g) * u).astype(BF16)
        if whole < width:
            left = width - whole
            gu = dot(z, jnp.concatenate([wg_ref[:, whole:], wu_ref[:, whole:]], axis=1))
            h_ref[:rows, whole:] = (jax.nn.silu(gu[:, :left]) * gu[:, left:]).astype(BF16)

    for rows in range(BLK, zs.shape[0] + 1, BLK):
        pl.when((total > rows - BLK) & (total <= rows))(functools.partial(block, rows))


def gate_up(n, off, nblk, w_gate, w_up, pos, xs, zs, most):
    experts, d, f = w_gate.shape
    ready, late, halves = len(zs), len(xs), len(xs[0])
    rows, tokens = zs[0].shape[0], sum(v.shape[0] for v in xs[0])
    return pl.pallas_call(
        functools.partial(gate_up_body, experts=experts, ready=ready, late=late, halves=halves),
        grid_spec=pltpu.PrefetchScalarGridSpec(
            num_scalar_prefetch=3,
            grid=(experts,),
            in_specs=[
                pl.BlockSpec((None, d, f), lambda e, *_: (e, 0, 0)),
                pl.BlockSpec((None, d, f), lambda e, *_: (e, 0, 0)),
            ]
            + [pl.BlockSpec(p.shape, lambda e, *_: (0, 0)) for p in pos]
            + [pl.BlockSpec(memory_space=pl.ANY)] * (late * halves + ready),
            out_specs=pl.BlockSpec((None, most, f), lambda e, *_: (e, 0, 0)),
            scratch_shapes=[
                pltpu.VMEM((late, tokens, d), BF16),
                pltpu.VMEM((ready + late, rows, d), BF16),
                pltpu.VMEM((most, d), BF16),
                pltpu.VMEM((2, BLK, tokens), BF16),
                pltpu.SemaphoreType.DMA((late, halves)),
                pltpu.SemaphoreType.DMA((ready,)),
            ],
        ),
        out_shape=jax.ShapeDtypeStruct((experts, most, f), BF16),
        compiler_params=pltpu.CompilerParams(vmem_limit_bytes=67_043_328),
        cost_estimate=cost(4 * experts * 256 * d * f, 2 * experts * d * f * 2),
        name="gate_up",
    )(n, off, nblk, w_gate, w_up, *pos, *[v for x in xs for v in x], *zs)


def comb_body(k_ref, pos_ref, gate_ref, c_ref):
    q = pl.program_id(0)
    tokens = c_ref.shape[1]

    def one(i, _):
        r = pl.ds(pl.multiple_of(i * 32, 32), 32)
        for t in range(0, tokens, 256):
            tile = c_ref.at[r, t : t + 256]
            tile[...] = picked(tile, slice(t, t + 256), i * 32, pos_ref, gate_ref)
        return _

    lax.fori_loop(0, k_ref[q] * (DEPTH // 32), one, 0)


def combine_matrices(k, pos, gate, rows):
    sources, top, tokens = pos.shape
    return pl.pallas_call(
        comb_body,
        grid_spec=pltpu.PrefetchScalarGridSpec(
            num_scalar_prefetch=1,
            grid=(sources,),
            in_specs=[pl.BlockSpec((None, top, tokens), lambda q, k: (q, 0, 0))] * 2,
            out_specs=pl.BlockSpec((None, rows, tokens), lambda q, k: (q, 0, 0)),
        ),
        out_shape=jax.ShapeDtypeStruct((sources, rows, tokens), BF16),
        compiler_params=pltpu.CompilerParams(vmem_limit_bytes=60 * MIB),
        cost_estimate=cost(4 * MIB, 8 * MIB),
        name="comb",
    )(k, pos, gate)


def combine(k, c, rows, out):
    deepest = rows.shape[0] // DEPTH

    def whole(depth):
        def part(i, _):
            t = pl.ds(pl.multiple_of(i * 512, 512), 512)
            both = (((0,), (0,)), ((), ()))
            out(t, lax.dot_general(c[:depth, t], rows[:depth, :], both, preferred_element_type=F32))
            return _

        lax.fori_loop(0, c.shape[1] // 512, part, 0)

    pl.when(k < deepest)(functools.partial(whole, (deepest - 1) * DEPTH))
    pl.when(k >= deepest)(functools.partial(whole, deepest * DEPTH))


def down_body(n_ref, off_ref, k_ref, wd_ref, h_ref, c_ref, *rest, experts, own, far, group):
    y_refs, own_ref, (hb, stage, outs, cb, sem, csem) = rest[-far - 7 : -7], rest[-7], rest[-6:]
    step = pl.program_id(0)
    sources = own + far

    def c_copy(i):
        return pltpu.make_async_copy(c_ref.at[own + i], cb.at[i], csem.at[i])

    def h_copy(e, b):
        r = pl.ds(pl.multiple_of(b * BLK, BLK), BLK)
        return pltpu.make_async_copy(h_ref.at[e, r, :], hb.at[e, r, :], sem.at[e])

    @pl.when(step == 0)
    def _():
        def fetch(e, _):
            def one(b, _):
                h_copy(e, b).start()
                return _

            lax.fori_loop(0, pl.cdiv(rows_of(n_ref, e, sources, experts), BLK), one, 0)
            return _

        lax.fori_loop(0, experts, fetch, 0)
        for i in range(far):
            c_copy(i).start()
        outs[...] = jnp.zeros_like(outs)
        own_ref[...] = jnp.zeros_like(own_ref)

    def expert(g, _):
        e = step * group + g
        total = rows_of(n_ref, e, sources, experts)
        blocks = pl.cdiv(total, BLK)

        def arrive(b, _):
            h_copy(e, b).wait()
            return _

        lax.fori_loop(0, blocks, arrive, 0)

        def compute(rows):
            stage[:rows, :] = dot(hb[e, :rows, :], wd_ref[g]).astype(BF16)

        for rows in range(BLK, stage.shape[0] + 1, BLK):
            pl.when(blocks == rows // BLK)(functools.partial(compute, rows))

        at = 0
        for q in range(sources):
            n = n_ref[q * experts + e]
            off = off_ref[q * experts + e]
            to = own_ref.at[q] if q < own else outs.at[q - own]

            def move(i, _):
                src = pl.ds(pl.multiple_of(at + i * ROW, ROW), ROW)
                dst = pl.ds(pl.multiple_of(off + i * ROW, ROW), ROW)
                to[dst, :] = stage[src, :]
                return _

            lax.fori_loop(0, n // ROW, move, 0)
            at = at + n
        return _

    lax.fori_loop(0, group, expert, 0)

    @pl.when(step == experts // group - 1)
    def _():
        for i in reversed(range(far)):
            c_copy(i).wait()

            def out(t, v):
                y_refs[i][t, :] = v.astype(y_refs[i].dtype)

            combine(k_ref[own + i], cb.at[i], outs.at[i], out)


def down(n, off, k, w_down, h, comb, kept, column, columns, own, group=1):
    experts, f, d = w_down.shape
    sources, rows, tokens = comb.shape
    far = sources - own
    most = h.shape[1]
    once = dict(pipeline_mode=pl.Buffered(1))
    at = column // columns
    aliased = [] if kept is None else [kept]
    return pl.pallas_call(
        functools.partial(down_body, experts=experts, own=own, far=far, group=group),
        grid_spec=pltpu.PrefetchScalarGridSpec(
            num_scalar_prefetch=3,
            grid=(experts // group,),
            in_specs=[pl.BlockSpec((group, f, columns), lambda e, *_: (e, 0, at))]
            + [pl.BlockSpec(memory_space=pl.ANY)] * (2 + len(aliased)),
            out_specs=[pl.BlockSpec((tokens, columns), lambda e, *_: (0, 0), **once)] * far
            + [pl.BlockSpec((own, rows, columns), lambda e, *_: (0, 0, at), **once)],
            scratch_shapes=[
                pltpu.VMEM((experts, most, f), BF16),
                pltpu.VMEM((most, columns), BF16),
                pltpu.VMEM((far, rows, columns), BF16),
                pltpu.VMEM((far, rows, tokens), BF16),
                pltpu.SemaphoreType.DMA((experts,)),
                pltpu.SemaphoreType.DMA((far,)),
            ],
        ),
        out_shape=[jax.ShapeDtypeStruct((tokens, columns), F32 if i == 0 else BF16) for i in range(far)]
        + [jax.ShapeDtypeStruct((own, rows, d), BF16)],
        input_output_aliases={6: far} if aliased else {},
        compiler_params=pltpu.CompilerParams(vmem_limit_bytes=67_043_328),
        cost_estimate=cost(2 * experts * 256 * f * columns, experts * f * columns * 2),
        name="down",
    )(n, off, k, w_down, h, comb, *aliased)


def own_body(k_ref, c_ref, r_ref, s_ref, *y_refs):
    for i in reversed(range(len(y_refs))):

        def out(t, v):
            y_refs[i][t, :] = v + s_ref[t, :] if i == 0 else v.astype(BF16)

        combine(k_ref[i], c_ref.at[i], r_ref.at[i], out)


def own_sums(k, comb, kept, shared, columns=512):
    own, rows, d = kept.shape
    tokens = comb.shape[2]
    return pl.pallas_call(
        own_body,
        grid_spec=pltpu.PrefetchScalarGridSpec(
            num_scalar_prefetch=1,
            grid=(d // columns,),
            in_specs=[
                pl.BlockSpec((own, rows, tokens), lambda c, *_: (0, 0, 0), pipeline_mode=pl.Buffered(1)),
                pl.BlockSpec((own, rows, columns), lambda c, *_: (0, 0, c)),
                pl.BlockSpec((tokens, columns), lambda c, *_: (0, c)),
            ],
            out_specs=[pl.BlockSpec((tokens, columns), lambda c, *_: (0, c))] * own,
        ),
        out_shape=[jax.ShapeDtypeStruct((tokens, d), F32 if i == 0 else BF16) for i in range(own)],
        compiler_params=pltpu.CompilerParams(vmem_limit_bytes=60 * MIB),
        cost_estimate=cost(4 * tokens * rows * d, 20 * MIB),
        name="own",
    )(k, comb, kept, shared)


def layer(x, expert, slot, gate, w_gate, w_up, w_down, s_gate, s_up, s_down, *, members, experts):
    x, expert, slot, gate = x[0, 0], expert[0, 0], slot[0, 0], gate[0, 0]
    tokens, d = x.shape
    local = w_gate.shape[0]
    slots = 5 * tokens * expert.shape[1] // (4 * experts)
    most_q = pl.cdiv(slots, ROW) * ROW
    rows = pl.cdiv(local * most_q, DEPTH) * DEPTH
    most = pl.cdiv(members * most_q, BLK) * BLK
    me = lax.axis_index("ep")

    def swap(v, q):
        return lax.ppermute(v, "ep", [(i, i ^ q) for i in range(members)])

    mark = (expert * 128 + jnp.minimum(slot, 127)).astype(F32)
    meta = jnp.stack([mark.T, gate.T])
    metas = [meta]
    for q in range(1, members):
        metas.append(swap(meta, q))
    metas = jnp.stack(metas)
    far = swap(x, 2)
    near = swap(x, 1)

    mark = metas[:, 0].astype(jnp.int32)
    where, s = (mark >> 7) - me * local, mark & 127
    ok = (where >= 0) & (where < local) & (s < slots)
    ids = jnp.arange(local, dtype=jnp.int32)
    is_it = (where[:, None] == ids[None, :, None, None]) & ok[:, None]
    n = jnp.max(jnp.where(is_it, s[:, None] + 1, 0), axis=(2, 3))
    n = (n + ROW - 1) // ROW * ROW
    off = jnp.sum(jnp.where(ids[None, :] < ids[:, None], n[:, None, :], 0), axis=2)
    used = jnp.sum(n, axis=1)
    pos = jnp.where(ok, jnp.sum(jnp.where(is_it, off[:, :, None, None], 0), axis=1) + s, -1).astype(F32)
    nf, of = n.reshape(-1), off.reshape(-1)
    nblk = (used + BLK - 1) // BLK
    k = jnp.maximum((used + DEPTH - 1) // DEPTH, rows // DEPTH - 1)

    def send(q, v):
        return dispatch(nblk[q : q + 1], pos[q], v, rows)

    chunks = s_gate.shape[1] // 512
    cut = chunks * 7 // 11
    y_shared = shared_expert(x, s_gate, s_up, s_down, 0, cut)
    z = [send(0, x), send(1, near)]
    far_near = swap(far, 1)
    comb = combine_matrices(k, pos, metas[:, 1].astype(BF16).astype(F32), rows)
    h = gate_up(nf, of, nblk, w_gate, w_up, [pos[2], pos[3]], [[far], [far_near]], z, most)

    back, kept, at = [], None, 0
    for columns in (d // 2, d // 2):
        y2, y3, kept = down(nf, of, k, w_down, h, comb, kept, at, columns, 2)
        mine = y2 + swap(y3, 1).astype(F32)
        back.append(swap(mine.astype(BF16), 2))
        at += columns
    y0, y1 = own_sums(k, comb, kept, y_shared)
    side = swap(y1, 1)
    y_shared = shared_expert(x, s_gate, s_up, s_down, cut, chunks, y0)
    return (y_shared + side.astype(F32) + jnp.concatenate(back, axis=1).astype(F32)).astype(BF16)[None, None]


def solution(mesh):
    members = mesh.shape["ep"]
    tok = P("dp", "ep", None, None)
    w = P("ep", None, None)
    rep = P(None, None)

    def step(x, expert, slot, gate, w_gate, w_up, w_down, s_gate, s_up, s_down):
        body = functools.partial(layer, members=members, experts=w_gate.shape[0])
        return jax.shard_map(
            body,
            mesh=mesh,
            in_specs=(tok, tok, tok, tok, w, w, w, rep, rep, rep),
            out_specs=tok,
            check_vma=False,
        )(x, expert, slot, gate, w_gate, w_up, w_down, s_gate, s_up, s_down)

    return step
```

```python
import functools

import jax
import jax.numpy as jnp
from jax import lax
from jax.experimental import pallas as pl
from jax.experimental.pallas import tpu as pltpu
from jax.sharding import PartitionSpec as P


MIB = 1 << 20
ROW = 16
BLK = 128
DEPTH = 512
F32, BF16 = jnp.float32, jnp.bfloat16


def dot(a, b):
    return jnp.dot(a, b, preferred_element_type=F32)


def cost(flops, nbytes):
    return pl.CostEstimate(flops=int(flops), bytes_accessed=int(nbytes), transcendentals=0)


def shared_body(*refs, rows, steps, more):
    if more:
        k_ref, x_ref, g_ref, u_ref, d_ref, init_ref, c_ref, r_ref, y_ref, ib, cb, rb, sem = refs
        copies = [
            pltpu.make_async_copy(init_ref, ib, sem.at[0]),
            pltpu.make_async_copy(c_ref.at[0], cb, sem.at[1]),
            pltpu.make_async_copy(r_ref.at[0], rb, sem.at[2]),
        ]
    else:
        x_ref, g_ref, u_ref, d_ref, y_ref = refs
    step = pl.program_id(0)
    tokens, width = x_ref.shape[0], g_ref.shape[1]
    depth = d_ref.shape[1]

    @pl.when(step == 0)
    def _():
        if more:
            for copy in copies:
                copy.start()
        y_ref[...] = jnp.zeros_like(y_ref)

    def one(i, _):
        r = pl.ds(pl.multiple_of(i * rows, rows), rows)
        x = x_ref[r, :]
        hs = []
        for c in range(0, width, 256):
            g = dot(x, g_ref[:, c : c + 256])
            u = dot(x, u_ref[:, c : c + 256])
            hs.append((jax.nn.silu(g) * u).astype(BF16))
        h = jnp.concatenate(hs, axis=1)
        for c in range(0, depth, 256):
            y_ref[r, c : c + 256] += dot(h, d_ref[:, c : c + 256])
        return _

    lax.fori_loop(0, tokens // rows, one, 0)

    if more:

        @pl.when(step == steps - 1)
        def _():
            for copy in copies:
                copy.wait()

            def out(t, c, v):
                y_ref[t, c] += v + ib[t, c]

            combine(k_ref[0], cb, rb, out)


def shared_expert(x, s_gate, s_up, s_down, first, last, more=None, chunk=512, rows=512):
    tokens, d = x.shape
    once = dict(pipeline_mode=pl.Buffered(1))
    scratch, rest = [], ()
    if more is not None:
        k, *rest = more
        _, comb, kept = rest
        scratch = [
            pltpu.VMEM((tokens, d), F32),
            pltpu.VMEM(comb.shape[1:], BF16),
            pltpu.VMEM(kept.shape[1:], BF16),
            pltpu.SemaphoreType.DMA((3,)),
        ]
    return pl.pallas_call(
        functools.partial(shared_body, rows=rows, steps=last - first, more=more is not None),
        grid_spec=pltpu.PrefetchScalarGridSpec(
            num_scalar_prefetch=0 if more is None else 1,
            grid=(last - first,),
            in_specs=[
                pl.BlockSpec((tokens, d), lambda i, *_: (0, 0), **once),
                pl.BlockSpec((d, chunk), lambda i, *_: (0, i + first)),
                pl.BlockSpec((d, chunk), lambda i, *_: (0, i + first)),
                pl.BlockSpec((chunk, d), lambda i, *_: (i + first, 0)),
            ]
            + [pl.BlockSpec(memory_space=pl.ANY)] * len(rest),
            out_specs=pl.BlockSpec((tokens, d), lambda i, *_: (0, 0), **once),
            scratch_shapes=scratch,
        ),
        out_shape=jax.ShapeDtypeStruct((tokens, d), F32),
        compiler_params=pltpu.CompilerParams(vmem_limit_bytes=60 * MIB),
        cost_estimate=cost(6 * tokens * d * chunk * (last - first), 6 * d * chunk * (last - first)),
        name="shared",
    )(*([] if more is None else [k]), x, s_gate, s_up, s_down, *rest)


def picked(values, tokens, first, pos, other=None):
    row = (first + lax.broadcasted_iota(jnp.int32, (values.shape[0], 1), 0)).astype(F32)
    tile = jnp.zeros(values.shape, F32)
    for j in range(pos.shape[0]):
        hit = jnp.broadcast_to(pos[j : j + 1, tokens], values.shape) == row
        tile = jnp.where(hit, 1.0 if other is None else other[j : j + 1, tokens], tile)
    return tile.astype(BF16)


def select_rows(pos, first, out):
    for r in range(0, out.shape[0], 32):
        for t in range(0, out.shape[1], 256):
            tile = out.at[r : r + 32, t : t + 256]
            tile[...] = picked(tile, slice(t, t + 256), first + r, pos)


def gather(count, pos, x, z, p, first=0):
    def one(i, _):
        select_rows(pos, (first + i + 1) * BLK, p.at[(i + 1) % 2])
        r = pl.ds(pl.multiple_of(i * BLK, BLK), BLK)
        for c in range(0, x.shape[1], 256):
            z[r, c : c + 256] = dot(p[i % 2], x[:, c : c + 256]).astype(BF16)
        return _

    pl.when(count > 0)(lambda: select_rows(pos, first * BLK, p.at[0]))
    lax.fori_loop(0, count, one, 0)


def dispatch_body(nblk_ref, pos_ref, x_ref, z_ref, p, *, group):
    step = pl.program_id(0)
    gather(jnp.clip(nblk_ref[0] - step * group, 0, group), pos_ref, x_ref, z_ref, p, step * group)


def dispatch(nblk, pos, x, rows, group=4):
    tokens, d = x.shape
    last = lambda b, n: jnp.minimum(b, jnp.maximum(pl.cdiv(n[0], group) - 1, 0))
    return pl.pallas_call(
        functools.partial(dispatch_body, group=group),
        grid_spec=pltpu.PrefetchScalarGridSpec(
            num_scalar_prefetch=1,
            grid=(rows // (BLK * group),),
            in_specs=[
                pl.BlockSpec(pos.shape, lambda b, n: (0, 0)),
                pl.BlockSpec((tokens, d), lambda b, n: (0, 0)),
            ],
            out_specs=pl.BlockSpec((BLK * group, d), lambda b, n: (last(b, n), 0)),
            scratch_shapes=[pltpu.VMEM((2, BLK, tokens), BF16)],
        ),
        out_shape=jax.ShapeDtypeStruct((rows, d), BF16),
        compiler_params=pltpu.CompilerParams(vmem_limit_bytes=60 * MIB),
        cost_estimate=cost(2 * tokens * d * rows // 3, 8 * MIB),
        name="dispatch",
    )(nblk, pos, x)


def rows_of(n_ref, e, sources, experts):
    total = 0
    for q in range(sources):
        total = total + n_ref[q * experts + e]
    return total


def gate_up_body(n_ref, off_ref, nblk_ref, wg_ref, wu_ref, *rest, experts, ready, late, halves):
    sources = ready + late
    pos_refs, rest = rest[:late], rest[late:]
    x_refs, rest = rest[: late * halves], rest[late * halves :]
    z_refs, (h_ref, xv, zv, zs, p, xsem, zsem) = rest[:ready], rest[ready:]
    e = pl.program_id(0)
    width = wg_ref.shape[1]

    def x_copy(i, j):
        size = x_refs[0].shape[0]
        return pltpu.make_async_copy(x_refs[i * halves + j], xv.at[i, pl.ds(j * size, size), :], xsem.at[i, j])

    def z_copy(q, b):
        r = pl.ds(pl.multiple_of(b * BLK, BLK), BLK)
        return pltpu.make_async_copy(z_refs[q].at[r, :], zv.at[q, r, :], zsem.at[q])

    @pl.when(e == 0)
    def _():
        for i in range(late):
            for j in range(halves):
                x_copy(i, j).start()

        def each(q, act):
            def one(b, _):
                act(z_copy(q, b))
                return _

            lax.fori_loop(0, nblk_ref[q], one, 0)

        for q in range(ready):
            each(q, lambda c: c.start())
        for i in range(late):
            for j in range(halves):
                x_copy(i, j).wait()
            q = ready + i

            gather(nblk_ref[q], pos_refs[i], xv.at[i], zv.at[q], p)
        for q in range(ready):
            each(q, lambda c: c.wait())

    at = 0
    for q in range(sources):
        n = n_ref[q * experts + e]
        off = off_ref[q * experts + e]

        def move(i, _):
            src = pl.ds(pl.multiple_of(off + i * ROW, ROW), ROW)
            dst = pl.ds(pl.multiple_of(at + i * ROW, ROW), ROW)
            zs[dst, :] = zv[q, src, :]
            return _

        lax.fori_loop(0, n // ROW, move, 0)
        at = at + n
    total = at

    def block(rows):
        z = zs[:rows, :]
        whole = width // 256 * 256
        for c in range(0, whole, 256):
            g = dot(z, wg_ref[:, c : c + 256])
            u = dot(z, wu_ref[:, c : c + 256])
            h_ref[:rows, c : c + 256] = (jax.nn.silu(g) * u).astype(BF16)
        if whole < width:
            left = width - whole
            gu = dot(z, jnp.concatenate([wg_ref[:, whole:], wu_ref[:, whole:]], axis=1))
            h_ref[:rows, whole:] = (jax.nn.silu(gu[:, :left]) * gu[:, left:]).astype(BF16)

    for rows in range(BLK, zs.shape[0] + 1, BLK):
        pl.when((total > rows - BLK) & (total <= rows))(functools.partial(block, rows))


def gate_up(n, off, nblk, w_gate, w_up, pos, xs, zs, most):
    experts, d, f = w_gate.shape
    ready, late, halves = len(zs), len(xs), len(xs[0])
    rows, tokens = zs[0].shape[0], sum(v.shape[0] for v in xs[0])
    return pl.pallas_call(
        functools.partial(gate_up_body, experts=experts, ready=ready, late=late, halves=halves),
        grid_spec=pltpu.PrefetchScalarGridSpec(
            num_scalar_prefetch=3,
            grid=(experts,),
            in_specs=[
                pl.BlockSpec((None, d, f), lambda e, *_: (e, 0, 0)),
                pl.BlockSpec((None, d, f), lambda e, *_: (e, 0, 0)),
            ]
            + [pl.BlockSpec(p.shape, lambda e, *_: (0, 0)) for p in pos]
            + [pl.BlockSpec(memory_space=pl.ANY)] * (late * halves + ready),
            out_specs=pl.BlockSpec((None, most, f), lambda e, *_: (e, 0, 0)),
            scratch_shapes=[
                pltpu.VMEM((late, tokens, d), BF16),
                pltpu.VMEM((ready + late, rows, d), BF16),
                pltpu.VMEM((most, d), BF16),
                pltpu.VMEM((2, BLK, tokens), BF16),
                pltpu.SemaphoreType.DMA((late, halves)),
                pltpu.SemaphoreType.DMA((ready,)),
            ],
        ),
        out_shape=jax.ShapeDtypeStruct((experts, most, f), BF16),
        compiler_params=pltpu.CompilerParams(vmem_limit_bytes=67_043_328),
        cost_estimate=cost(4 * experts * 256 * d * f, 2 * experts * d * f * 2),
        name="gate_up",
    )(n, off, nblk, w_gate, w_up, *pos, *[v for x in xs for v in x], *zs)


def comb_body(k_ref, pos_ref, gate_ref, c_ref):
    q = pl.program_id(0)
    tokens = c_ref.shape[1]

    def one(i, _):
        r = pl.ds(pl.multiple_of(i * 32, 32), 32)
        for t in range(0, tokens, 256):
            tile = c_ref.at[r, t : t + 256]
            tile[...] = picked(tile, slice(t, t + 256), i * 32, pos_ref, gate_ref)
        return _

    lax.fori_loop(0, k_ref[q] * (DEPTH // 32), one, 0)


def combine_matrices(k, pos, gate, rows):
    sources, top, tokens = pos.shape
    return pl.pallas_call(
        comb_body,
        grid_spec=pltpu.PrefetchScalarGridSpec(
            num_scalar_prefetch=1,
            grid=(sources,),
            in_specs=[pl.BlockSpec((None, top, tokens), lambda q, k: (q, 0, 0))] * 2,
            out_specs=pl.BlockSpec((None, rows, tokens), lambda q, k: (q, 0, 0)),
        ),
        out_shape=jax.ShapeDtypeStruct((sources, rows, tokens), BF16),
        compiler_params=pltpu.CompilerParams(vmem_limit_bytes=60 * MIB),
        cost_estimate=cost(4 * MIB, 8 * MIB),
        name="comb",
    )(k, pos, gate)


def combine(k, c, rows, out):
    deepest = rows.shape[0] // DEPTH

    def whole(depth):
        def part(i, _):
            t = pl.ds(pl.multiple_of(i * 256, 256), 256)
            both = (((0,), (0,)), ((), ()))
            for n in range(0, rows.shape[1], 256):
                n = slice(n, n + 256)
                out(t, n, lax.dot_general(c[:depth, t], rows[:depth, n], both, preferred_element_type=F32))
            return _

        lax.fori_loop(0, c.shape[1] // 256, part, 0)

    pl.when(k < deepest)(functools.partial(whole, (deepest - 1) * DEPTH))
    pl.when(k >= deepest)(functools.partial(whole, deepest * DEPTH))


def down_body(n_ref, off_ref, k_ref, wd_ref, h_ref, c_ref, *rest, experts, own, far, group, column):
    y_refs, kept_ref, (hb, stage, outs, cb, sem, csem, osem) = rest[-far - 8 : -8], rest[-8], rest[-7:]
    step = pl.program_id(0)
    sources = own + far

    def c_copy(i):
        return pltpu.make_async_copy(c_ref.at[own + i], cb.at[i], csem.at[i])

    def h_copy(e, b):
        r = pl.ds(pl.multiple_of(b * BLK, BLK), BLK)
        return pltpu.make_async_copy(h_ref.at[e, r, :], hb.at[e, r, :], sem.at[e])

    @pl.when(step == 0)
    def _():
        def fetch(e, _):
            def one(b, _):
                h_copy(e, b).start()
                return _

            lax.fori_loop(0, pl.cdiv(rows_of(n_ref, e, sources, experts), BLK), one, 0)
            return _

        lax.fori_loop(0, experts, fetch, 0)
        for i in range(far):
            c_copy(i).start()
        zeros = jnp.zeros((ROW, outs.shape[2]), BF16)
        for q in range(sources):
            used = off_ref[(q + 1) * experts - 1] + n_ref[(q + 1) * experts - 1]

            def clear(i, _):
                outs[q, pl.ds(pl.multiple_of(i * ROW, ROW), ROW), :] = zeros
                return _

            lax.fori_loop(used // ROW, outs.shape[1] // ROW, clear, 0)

    def expert(g, _):
        e = step * group + g
        total = rows_of(n_ref, e, sources, experts)
        blocks = pl.cdiv(total, BLK)

        def arrive(b, _):
            h_copy(e, b).wait()
            return _

        lax.fori_loop(0, blocks, arrive, 0)

        def compute(rows):
            stage[:rows, :] = dot(hb[e, :rows, :], wd_ref[g]).astype(BF16)

        for rows in range(BLK, stage.shape[0] + 1, BLK):
            pl.when(blocks == rows // BLK)(functools.partial(compute, rows))

        at = 0
        for q in range(sources):
            n = n_ref[q * experts + e]
            off = off_ref[q * experts + e]

            def move(i, _):
                src = pl.ds(pl.multiple_of(at + i * ROW, ROW), ROW)
                dst = pl.ds(pl.multiple_of(off + i * ROW, ROW), ROW)
                outs[q, dst, :] = stage[src, :]
                return _

            lax.fori_loop(0, n // ROW, move, 0)
            at = at + n
        return _

    lax.fori_loop(0, group, expert, 0)

    @pl.when(step == experts // group - 1)
    def _():
        columns = pl.ds(column, outs.shape[2])
        leave = pltpu.make_async_copy(outs.at[:own], kept_ref.at[:, :, columns], osem)
        leave.start()
        for i in reversed(range(far)):
            c_copy(i).wait()

            def out(t, c, v):
                y_refs[i][t, c] = v.astype(y_refs[i].dtype)

            combine(k_ref[own + i], cb.at[i], outs.at[own + i], out)
        leave.wait()


def down(n, off, k, w_down, h, comb, kept, column, columns, own, group=3):
    experts, f, d = w_down.shape
    sources, rows, tokens = comb.shape
    far = sources - own
    most = h.shape[1]
    once = dict(pipeline_mode=pl.Buffered(1))
    at = column // columns
    aliased = [] if kept is None else [kept]
    return pl.pallas_call(
        functools.partial(down_body, experts=experts, own=own, far=far, group=group, column=column),
        grid_spec=pltpu.PrefetchScalarGridSpec(
            num_scalar_prefetch=3,
            grid=(experts // group,),
            in_specs=[pl.BlockSpec((group, f, columns), lambda e, *_: (e, 0, at))]
            + [pl.BlockSpec(memory_space=pl.ANY)] * (2 + len(aliased)),
            out_specs=[pl.BlockSpec((tokens, columns), lambda e, *_: (0, 0), **once)] * far
            + [pl.BlockSpec(memory_space=pl.ANY)],
            scratch_shapes=[
                pltpu.VMEM((experts, most, f), BF16),
                pltpu.VMEM((most, columns), BF16),
                pltpu.VMEM((sources, rows, columns), BF16),
                pltpu.VMEM((far, rows, tokens), BF16),
                pltpu.SemaphoreType.DMA((experts,)),
                pltpu.SemaphoreType.DMA((far,)),
                pltpu.SemaphoreType.DMA,
            ],
        ),
        out_shape=[jax.ShapeDtypeStruct((tokens, columns), F32 if i == 0 else BF16) for i in range(far)]
        + [jax.ShapeDtypeStruct((own, rows, d), BF16)],
        input_output_aliases={6: far} if aliased else {},
        compiler_params=pltpu.CompilerParams(vmem_limit_bytes=67_043_328),
        cost_estimate=cost(2 * experts * 256 * f * columns, experts * f * columns * 2),
        name="down",
    )(n, off, k, w_down, h, comb, *aliased)


def side_body(k_ref, c_ref, r_ref, y_ref, *, member):
    def out(t, c, v):
        y_ref[t, c] = v.astype(BF16)

    combine(k_ref[member], c_ref, r_ref, out)


def side_sums(k, comb, kept, member, columns=1024):
    own, rows, d = kept.shape
    tokens = comb.shape[2]
    return pl.pallas_call(
        functools.partial(side_body, member=member),
        grid_spec=pltpu.PrefetchScalarGridSpec(
            num_scalar_prefetch=1,
            grid=(d // columns,),
            in_specs=[
                pl.BlockSpec((None, rows, tokens), lambda c, *_: (member, 0, 0), pipeline_mode=pl.Buffered(1)),
                pl.BlockSpec((None, rows, columns), lambda c, *_: (member, 0, c)),
            ],
            out_specs=pl.BlockSpec((tokens, columns), lambda c, *_: (0, c)),
        ),
        out_shape=jax.ShapeDtypeStruct((tokens, d), BF16),
        compiler_params=pltpu.CompilerParams(vmem_limit_bytes=60 * MIB),
        cost_estimate=cost(2 * tokens * rows * d, 14 * MIB),
        name="side",
    )(k, comb, kept)


def layer(x, expert, slot, gate, w_gate, w_up, w_down, s_gate, s_up, s_down, *, members, experts):
    x, expert, slot, gate = x[0, 0], expert[0, 0], slot[0, 0], gate[0, 0]
    tokens, d = x.shape
    local = w_gate.shape[0]
    slots = 5 * tokens * expert.shape[1] // (4 * experts)
    most_q = pl.cdiv(slots, ROW) * ROW
    rows = pl.cdiv(local * most_q, DEPTH) * DEPTH
    most = pl.cdiv(members * most_q, BLK) * BLK
    me = lax.axis_index("ep")

    def swap(v, q):
        return lax.ppermute(v, "ep", [(i, i ^ q) for i in range(members)])

    mark = (expert * 128 + jnp.minimum(slot, 127)).astype(F32)
    meta = jnp.stack([mark.T, gate.T])
    metas = [meta]
    for q in range(1, members):
        metas.append(swap(meta, q))
    metas = jnp.stack(metas)
    far = swap(x, 2)
    near = swap(x, 1)

    mark = metas[:, 0].astype(jnp.int32)
    where, s = (mark >> 7) - me * local, mark & 127
    ok = (where >= 0) & (where < local) & (s < slots)
    ids = jnp.arange(local, dtype=jnp.int32)
    is_it = (where[:, None] == ids[None, :, None, None]) & ok[:, None]
    n = jnp.max(jnp.where(is_it, s[:, None] + 1, 0), axis=(2, 3))
    n = (n + ROW - 1) // ROW * ROW
    off = jnp.sum(jnp.where(ids[None, :] < ids[:, None], n[:, None, :], 0), axis=2)
    used = jnp.sum(n, axis=1)
    pos = jnp.where(ok, jnp.sum(jnp.where(is_it, off[:, :, None, None], 0), axis=1) + s, -1).astype(F32)
    nf, of = n.reshape(-1), off.reshape(-1)
    nblk = (used + BLK - 1) // BLK
    k = jnp.maximum((used + DEPTH - 1) // DEPTH, rows // DEPTH - 1)

    def send(q, v):
        return dispatch(nblk[q : q + 1], pos[q], v, rows)

    chunks = s_gate.shape[1] // 512
    cut = chunks * 8 // 11
    y_shared = shared_expert(x, s_gate, s_up, s_down, 0, cut)
    z = [send(0, x), send(1, near)]
    far_near = swap(far, 1)
    comb = combine_matrices(k, pos, metas[:, 1].astype(BF16).astype(F32), rows)
    h = gate_up(nf, of, nblk, w_gate, w_up, [pos[2], pos[3]], [[far], [far_near]], z, most)

    back, kept, at = [], None, 0
    for columns in (d // 2, d // 2):
        y2, y3, kept = down(nf, of, k, w_down, h, comb, kept, at, columns, 2)
        mine = y2 + swap(y3, 1).astype(F32)
        back.append(swap(mine.astype(BF16), 2))
        at += columns
    y1 = side_sums(k, comb, kept, 1)
    side = swap(y1, 1)
    y_shared = shared_expert(x, s_gate, s_up, s_down, cut, chunks, (k, y_shared, comb, kept))
    return (y_shared + side.astype(F32) + jnp.concatenate(back, axis=1).astype(F32)).astype(BF16)[None, None]


def solution(mesh):
    members = mesh.shape["ep"]
    tok = P("dp", "ep", None, None)
    w = P("ep", None, None)
    rep = P(None, None)

    def step(x, expert, slot, gate, w_gate, w_up, w_down, s_gate, s_up, s_down):
        body = functools.partial(layer, members=members, experts=w_gate.shape[0])
        return jax.shard_map(
            body,
            mesh=mesh,
            in_specs=(tok, tok, tok, tok, w, w, w, rep, rep, rep),
            out_specs=tok,
            check_vma=False,
        )(x, expert, slot, gate, w_gate, w_up, w_down, s_gate, s_up, s_down)

    return step
```

```python
import functools

import jax
import jax.numpy as jnp
from jax import lax
from jax.experimental import pallas as pl
from jax.experimental.pallas import tpu as pltpu
from jax.sharding import PartitionSpec as P


MIB = 1 << 20
ROW = 16
BLK = 128
DEPTH = 512
F32, BF16 = jnp.float32, jnp.bfloat16


def dot(a, b):
    return jnp.dot(a, b, preferred_element_type=F32)


def cost(flops, nbytes):
    return pl.CostEstimate(flops=int(flops), bytes_accessed=int(nbytes), transcendentals=0)


def shared_body(*refs, rows, steps, more):
    if more:
        k_ref, x_ref, g_ref, u_ref, d_ref, init_ref, c_ref, r_ref, y_ref, ib, cb, rb, sem = refs
        copies = [
            pltpu.make_async_copy(init_ref, ib, sem.at[0]),
            pltpu.make_async_copy(c_ref.at[0], cb, sem.at[1]),
            pltpu.make_async_copy(r_ref.at[0], rb, sem.at[2]),
        ]
    else:
        x_ref, g_ref, u_ref, d_ref, y_ref = refs
    step = pl.program_id(0)
    tokens, width = x_ref.shape[0], g_ref.shape[1]
    depth = d_ref.shape[1]

    @pl.when(step == 0)
    def _():
        if more:
            for copy in copies:
                copy.start()
        y_ref[...] = jnp.zeros_like(y_ref)

    def one(i, _):
        r = pl.ds(pl.multiple_of(i * rows, rows), rows)
        x = x_ref[r, :]
        hs = []
        for c in range(0, width, 256):
            g = dot(x, g_ref[:, c : c + 256])
            u = dot(x, u_ref[:, c : c + 256])
            hs.append((jax.nn.silu(g) * u).astype(BF16))
        h = jnp.concatenate(hs, axis=1)
        for c in range(0, depth, 256):
            y_ref[r, c : c + 256] += dot(h, d_ref[:, c : c + 256])
        return _

    lax.fori_loop(0, tokens // rows, one, 0)

    if more:

        @pl.when(step == steps - 1)
        def _():
            for copy in copies:
                copy.wait()

            def out(t, c, v):
                y_ref[t, c] += v + ib[t, c]

            combine(k_ref[0], cb, rb, out)


def shared_expert(x, s_gate, s_up, s_down, first, last, more=None, chunk=512, rows=512):
    tokens, d = x.shape
    once = dict(pipeline_mode=pl.Buffered(1))
    scratch, rest = [], ()
    if more is not None:
        k, *rest = more
        _, comb, kept = rest
        scratch = [
            pltpu.VMEM((tokens, d), F32),
            pltpu.VMEM(comb.shape[1:], BF16),
            pltpu.VMEM(kept.shape[1:], BF16),
            pltpu.SemaphoreType.DMA((3,)),
        ]
    return pl.pallas_call(
        functools.partial(shared_body, rows=rows, steps=last - first, more=more is not None),
        grid_spec=pltpu.PrefetchScalarGridSpec(
            num_scalar_prefetch=0 if more is None else 1,
            grid=(last - first,),
            in_specs=[
                pl.BlockSpec((tokens, d), lambda i, *_: (0, 0), **once),
                pl.BlockSpec((d, chunk), lambda i, *_: (0, i + first)),
                pl.BlockSpec((d, chunk), lambda i, *_: (0, i + first)),
                pl.BlockSpec((chunk, d), lambda i, *_: (i + first, 0)),
            ]
            + [pl.BlockSpec(memory_space=pl.ANY)] * len(rest),
            out_specs=pl.BlockSpec((tokens, d), lambda i, *_: (0, 0), **once),
            scratch_shapes=scratch,
        ),
        out_shape=jax.ShapeDtypeStruct((tokens, d), F32),
        compiler_params=pltpu.CompilerParams(vmem_limit_bytes=60 * MIB),
        cost_estimate=cost(6 * tokens * d * chunk * (last - first), 6 * d * chunk * (last - first)),
        name="shared",
    )(*([] if more is None else [k]), x, s_gate, s_up, s_down, *rest)


def picked(values, tokens, first, pos, other=None):
    row = (first + lax.broadcasted_iota(jnp.int32, (values.shape[0], 1), 0)).astype(F32)
    tile = jnp.zeros(values.shape, F32)
    for j in range(pos.shape[0]):
        hit = jnp.broadcast_to(pos[j : j + 1, tokens], values.shape) == row
        tile = jnp.where(hit, 1.0 if other is None else other[j : j + 1, tokens], tile)
    return tile.astype(BF16)


def select_rows(pos, first, out):
    for r in range(0, out.shape[0], 32):
        for t in range(0, out.shape[1], 256):
            tile = out.at[r : r + 32, t : t + 256]
            tile[...] = picked(tile, slice(t, t + 256), first + r, pos)


def gather(count, pos, x, z, p, first=0):
    def one(i, _):
        select_rows(pos, (first + i + 1) * BLK, p.at[(i + 1) % 2])
        r = pl.ds(pl.multiple_of(i * BLK, BLK), BLK)
        for c in range(0, x.shape[1], 256):
            z[r, c : c + 256] = dot(p[i % 2], x[:, c : c + 256]).astype(BF16)
        return _

    pl.when(count > 0)(lambda: select_rows(pos, first * BLK, p.at[0]))
    lax.fori_loop(0, count, one, 0)


def dispatch_body(nblk_ref, pos_ref, x_ref, z_ref, p, *, group):
    step = pl.program_id(0)
    gather(jnp.clip(nblk_ref[0] - step * group, 0, group), pos_ref, x_ref, z_ref, p, step * group)


def dispatch(nblk, pos, x, rows, group=4):
    tokens, d = x.shape
    last = lambda b, n: jnp.minimum(b, jnp.maximum(pl.cdiv(n[0], group) - 1, 0))
    return pl.pallas_call(
        functools.partial(dispatch_body, group=group),
        grid_spec=pltpu.PrefetchScalarGridSpec(
            num_scalar_prefetch=1,
            grid=(rows // (BLK * group),),
            in_specs=[
                pl.BlockSpec(pos.shape, lambda b, n: (0, 0)),
                pl.BlockSpec((tokens, d), lambda b, n: (0, 0)),
            ],
            out_specs=pl.BlockSpec((BLK * group, d), lambda b, n: (last(b, n), 0)),
            scratch_shapes=[pltpu.VMEM((2, BLK, tokens), BF16)],
        ),
        out_shape=jax.ShapeDtypeStruct((rows, d), BF16),
        compiler_params=pltpu.CompilerParams(vmem_limit_bytes=60 * MIB),
        cost_estimate=cost(2 * tokens * d * rows // 3, 8 * MIB),
        name="dispatch",
    )(nblk, pos, x)


def rows_of(n_ref, e, sources, experts):
    total = 0
    for q in range(sources):
        total = total + n_ref[q * experts + e]
    return total


def gate_up_body(n_ref, off_ref, nblk_ref, wg_ref, wu_ref, *rest, experts, ready, late, halves, parts):
    sources = ready + late
    pos_refs, rest = rest[:late], rest[late:]
    x_refs, rest = rest[: late * halves], rest[late * halves :]
    z_refs, (h_ref, xv, zv, zs, p, wb, xsem, zsem, wsem) = rest[:ready], rest[ready:]
    e = pl.program_id(0)
    slot = e % 2

    def w_copies(e, part):
        columns = slice(*parts[part])
        for i, w_ref in enumerate((wg_ref, wu_ref)):
            to = wb.at[e % 2, i, :, columns]
            yield pltpu.make_async_copy(w_ref.at[e, :, columns], to, wsem.at[e % 2, part, i])

    @pl.when(e == 0)
    def _():
        for first in range(2):
            for part in range(len(parts)):
                for copy in w_copies(first, part):
                    copy.start()

    def x_copy(i, j):
        size = x_refs[0].shape[0]
        return pltpu.make_async_copy(x_refs[i * halves + j], xv.at[i, pl.ds(j * size, size), :], xsem.at[i, j])

    def z_copy(q, b):
        r = pl.ds(pl.multiple_of(b * BLK, BLK), BLK)
        return pltpu.make_async_copy(z_refs[q].at[r, :], zv.at[q, r, :], zsem.at[q])

    @pl.when(e == 0)
    def _():
        for i in range(late):
            for j in range(halves):
                x_copy(i, j).start()

        def each(q, act):
            def one(b, _):
                act(z_copy(q, b))
                return _

            lax.fori_loop(0, nblk_ref[q], one, 0)

        for q in range(ready):
            each(q, lambda c: c.start())
        for i in range(late):
            for j in range(halves):
                x_copy(i, j).wait()
            q = ready + i

            gather(nblk_ref[q], pos_refs[i], xv.at[i], zv.at[q], p)
        for q in range(ready):
            each(q, lambda c: c.wait())

    at = 0
    for q in range(sources):
        n = n_ref[q * experts + e]
        off = off_ref[q * experts + e]

        def move(i, _):
            src = pl.ds(pl.multiple_of(off + i * ROW, ROW), ROW)
            dst = pl.ds(pl.multiple_of(at + i * ROW, ROW), ROW)
            zs[dst, :] = zv[q, src, :]
            return _

        lax.fori_loop(0, n // ROW, move, 0)
        at = at + n
    total = at

    def block(first, last, rows):
        z = zs[:rows, :]
        whole = first + (last - first) // 256 * 256
        for c in range(first, whole, 256):
            c = slice(c, c + 256)
            g = dot(z, wb[slot, 0, :, c])
            u = dot(z, wb[slot, 1, :, c])
            h_ref[:rows, c] = (jax.nn.silu(g) * u).astype(BF16)
        if whole < last:
            left, c = last - whole, slice(whole, last)
            gu = dot(z, jnp.concatenate([wb[slot, 0, :, c], wb[slot, 1, :, c]], axis=1))
            h_ref[:rows, c] = (jax.nn.silu(gu[:, :left]) * gu[:, left:]).astype(BF16)

    for part, (first, last) in enumerate(parts):
        for copy in w_copies(e, part):
            copy.wait()
        for rows in range(BLK, zs.shape[0] + 1, BLK):
            pl.when((total > rows - BLK) & (total <= rows))(functools.partial(block, first, last, rows))

        @pl.when(e + 2 < experts)
        def _():
            for copy in w_copies(e + 2, part):
                copy.start()


def gate_up(n, off, nblk, w_gate, w_up, pos, xs, zs, most):
    experts, d, f = w_gate.shape
    ready, late, halves = len(zs), len(xs), len(xs[0])
    rows, tokens = zs[0].shape[0], sum(v.shape[0] for v in xs[0])
    half = pl.cdiv(f, 512) * 256
    parts = ((0, half), (half, f))
    return pl.pallas_call(
        functools.partial(gate_up_body, experts=experts, ready=ready, late=late, halves=halves, parts=parts),
        grid_spec=pltpu.PrefetchScalarGridSpec(
            num_scalar_prefetch=3,
            grid=(experts,),
            in_specs=[pl.BlockSpec(memory_space=pl.ANY)] * 2
            + [pl.BlockSpec(p.shape, lambda e, *_: (0, 0)) for p in pos]
            + [pl.BlockSpec(memory_space=pl.ANY)] * (late * halves + ready),
            out_specs=pl.BlockSpec((None, most, f), lambda e, *_: (e, 0, 0)),
            scratch_shapes=[
                pltpu.VMEM((late, tokens, d), BF16),
                pltpu.VMEM((ready + late, rows, d), BF16),
                pltpu.VMEM((most, d), BF16),
                pltpu.VMEM((2, BLK, tokens), BF16),
                pltpu.VMEM((2, 2, d, f), BF16),
                pltpu.SemaphoreType.DMA((late, halves)),
                pltpu.SemaphoreType.DMA((ready,)),
                pltpu.SemaphoreType.DMA((2, len(parts), 2)),
            ],
        ),
        out_shape=jax.ShapeDtypeStruct((experts, most, f), BF16),
        compiler_params=pltpu.CompilerParams(vmem_limit_bytes=67_043_328),
        cost_estimate=cost(4 * experts * 256 * d * f, 2 * experts * d * f * 2),
        name="gate_up",
    )(n, off, nblk, w_gate, w_up, *pos, *[v for x in xs for v in x], *zs)


def comb_body(k_ref, pos_ref, gate_ref, c_ref):
    q = pl.program_id(0)
    tokens = c_ref.shape[1]

    def one(i, _):
        r = pl.ds(pl.multiple_of(i * 32, 32), 32)
        for t in range(0, tokens, 256):
            tile = c_ref.at[r, t : t + 256]
            tile[...] = picked(tile, slice(t, t + 256), i * 32, pos_ref, gate_ref)
        return _

    lax.fori_loop(0, k_ref[q] * (DEPTH // 32), one, 0)


def combine_matrices(k, pos, gate, rows):
    sources, top, tokens = pos.shape
    return pl.pallas_call(
        comb_body,
        grid_spec=pltpu.PrefetchScalarGridSpec(
            num_scalar_prefetch=1,
            grid=(sources,),
            in_specs=[pl.BlockSpec((None, top, tokens), lambda q, k: (q, 0, 0))] * 2,
            out_specs=pl.BlockSpec((None, rows, tokens), lambda q, k: (q, 0, 0)),
        ),
        out_shape=jax.ShapeDtypeStruct((sources, rows, tokens), BF16),
        compiler_params=pltpu.CompilerParams(vmem_limit_bytes=60 * MIB),
        cost_estimate=cost(4 * MIB, 8 * MIB),
        name="comb",
    )(k, pos, gate)


def combine(k, mat, rows, out):
    deepest = rows.shape[0] // DEPTH

    def whole(depth):
        groups = rows.shape[1] // 1024
        both = (((0,), (0,)), ((), ()))

        def part(i, _):
            t = pl.ds(pl.multiple_of(i // groups * 256, 256), 256)
            for c in range(4):
                n = pl.ds(pl.multiple_of(i % groups * 1024 + c * 256, 256), 256)
                out(t, n, lax.dot_general(mat[:depth, t], rows[:depth, n], both, preferred_element_type=F32))
            return _

        lax.fori_loop(0, mat.shape[1] // 256 * groups, part, 0)

    pl.when(k < deepest)(functools.partial(whole, (deepest - 1) * DEPTH))
    pl.when(k >= deepest)(functools.partial(whole, deepest * DEPTH))


def down_body(n_ref, off_ref, k_ref, wd_ref, h_ref, c_ref, *rest, experts, own, far, column):
    y_refs, kept_ref, (hb, stage, outs, cb, wb, sem, csem, osem, wsem) = rest[-far - 10 : -10], rest[-10], rest[-9:]
    sources, slots = own + far, wb.shape[0]
    columns = pl.ds(column, outs.shape[2])

    def c_copy(i):
        return pltpu.make_async_copy(c_ref.at[own + i], cb.at[i], csem.at[i])

    def h_copy(e, b):
        r = pl.ds(pl.multiple_of(b * BLK, BLK), BLK)
        return pltpu.make_async_copy(h_ref.at[e, r, :], hb.at[e, r, :], sem.at[e])

    def w_copy(e):
        return pltpu.make_async_copy(wd_ref.at[e, :, columns], wb.at[e % slots], wsem.at[e % slots])

    for e in range(slots):
        w_copy(e).start()

    def fetch(e, _):
        def one(b, _):
            h_copy(e, b).start()
            return _

        lax.fori_loop(0, pl.cdiv(rows_of(n_ref, e, sources, experts), BLK), one, 0)
        return _

    lax.fori_loop(0, experts, fetch, 0)
    for i in range(far):
        c_copy(i).start()
    zeros = jnp.zeros((ROW, outs.shape[2]), BF16)
    for q in range(sources):
        used = off_ref[(q + 1) * experts - 1] + n_ref[(q + 1) * experts - 1]

        def clear(i, _):
            outs[q, pl.ds(pl.multiple_of(i * ROW, ROW), ROW), :] = zeros
            return _

        lax.fori_loop(used // ROW, outs.shape[1] // ROW, clear, 0)

    def expert(e, _):
        total = rows_of(n_ref, e, sources, experts)
        blocks = pl.cdiv(total, BLK)

        def arrive(b, _):
            h_copy(e, b).wait()
            return _

        lax.fori_loop(0, blocks, arrive, 0)
        w_copy(e).wait()

        def compute(rows):
            stage[:rows, :] = dot(hb[e, :rows, :], wb[e % slots]).astype(BF16)

        for rows in range(BLK, stage.shape[0] + 1, BLK):
            pl.when(blocks == rows // BLK)(functools.partial(compute, rows))

        @pl.when(e + slots < experts)
        def more():
            w_copy(e + slots).start()

        at = 0
        for q in range(sources):
            n = n_ref[q * experts + e]
            off = off_ref[q * experts + e]

            def move(i, _):
                src = pl.ds(pl.multiple_of(at + i * ROW, ROW), ROW)
                dst = pl.ds(pl.multiple_of(off + i * ROW, ROW), ROW)
                outs[q, dst, :] = stage[src, :]
                return _

            lax.fori_loop(0, n // ROW, move, 0)
            at = at + n
        return _

    lax.fori_loop(0, experts, expert, 0)

    leave = pltpu.make_async_copy(outs.at[:own], kept_ref.at[:, :, columns], osem)
    leave.start()
    for i in reversed(range(far)):
        c_copy(i).wait()

        def out(t, c, v):
            y_refs[i][t, c] = v.astype(y_refs[i].dtype)

        combine(k_ref[own + i], cb.at[i], outs.at[own + i], out)
    leave.wait()


def down(n, off, k, w_down, h, comb, kept, column, columns, own, slots=6):
    experts, f, d = w_down.shape
    sources, rows, tokens = comb.shape
    far = sources - own
    most = h.shape[1]
    once = dict(pipeline_mode=pl.Buffered(1))
    aliased = [] if kept is None else [kept]
    return pl.pallas_call(
        functools.partial(down_body, experts=experts, own=own, far=far, column=column),
        grid_spec=pltpu.PrefetchScalarGridSpec(
            num_scalar_prefetch=3,
            grid=(1,),
            in_specs=[pl.BlockSpec(memory_space=pl.ANY)] * (3 + len(aliased)),
            out_specs=[pl.BlockSpec((tokens, columns), lambda e, *_: (0, 0), **once)] * far
            + [pl.BlockSpec(memory_space=pl.ANY)],
            scratch_shapes=[
                pltpu.VMEM((experts, most, f), BF16),
                pltpu.VMEM((most, columns), BF16),
                pltpu.VMEM((sources, rows, columns), BF16),
                pltpu.VMEM((far, rows, tokens), BF16),
                pltpu.VMEM((slots, f, columns), BF16),
                pltpu.SemaphoreType.DMA((experts,)),
                pltpu.SemaphoreType.DMA((far,)),
                pltpu.SemaphoreType.DMA,
                pltpu.SemaphoreType.DMA((slots,)),
            ],
        ),
        out_shape=[jax.ShapeDtypeStruct((tokens, columns), F32 if i == 0 else BF16) for i in range(far)]
        + [jax.ShapeDtypeStruct((own, rows, d), BF16)],
        input_output_aliases={6: far} if aliased else {},
        compiler_params=pltpu.CompilerParams(vmem_limit_bytes=67_043_328),
        cost_estimate=cost(2 * experts * 256 * f * columns, experts * f * columns * 2),
        name="down",
    )(n, off, k, w_down, h, comb, *aliased)


def side_body(k_ref, c_ref, r_ref, y_ref, *, member):
    def out(t, c, v):
        y_ref[t, c] = v.astype(BF16)

    combine(k_ref[member], c_ref, r_ref, out)


def side_sums(k, comb, kept, member, columns=1024):
    own, rows, d = kept.shape
    tokens = comb.shape[2]
    return pl.pallas_call(
        functools.partial(side_body, member=member),
        grid_spec=pltpu.PrefetchScalarGridSpec(
            num_scalar_prefetch=1,
            grid=(d // columns,),
            in_specs=[
                pl.BlockSpec((None, rows, tokens), lambda c, *_: (member, 0, 0), pipeline_mode=pl.Buffered(1)),
                pl.BlockSpec((None, rows, columns), lambda c, *_: (member, 0, c)),
            ],
            out_specs=pl.BlockSpec((tokens, columns), lambda c, *_: (0, c)),
        ),
        out_shape=jax.ShapeDtypeStruct((tokens, d), BF16),
        compiler_params=pltpu.CompilerParams(vmem_limit_bytes=60 * MIB),
        cost_estimate=cost(2 * tokens * rows * d, 14 * MIB),
        name="side",
    )(k, comb, kept)


def layer(x, expert, slot, gate, w_gate, w_up, w_down, s_gate, s_up, s_down, *, members, experts):
    x, expert, slot, gate = x[0, 0], expert[0, 0], slot[0, 0], gate[0, 0]
    tokens, d = x.shape
    local = w_gate.shape[0]
    slots = 5 * tokens * expert.shape[1] // (4 * experts)
    most_q = pl.cdiv(slots, ROW) * ROW
    rows = pl.cdiv(local * most_q, DEPTH) * DEPTH
    most = pl.cdiv(members * most_q, BLK) * BLK
    me = lax.axis_index("ep")

    def swap(v, q):
        return lax.ppermute(v, "ep", [(i, i ^ q) for i in range(members)])

    mark = (expert * 128 + jnp.minimum(slot, 127)).astype(F32)
    meta = jnp.stack([mark.T, gate.T])
    metas = [meta]
    for q in range(1, members):
        metas.append(swap(meta, q))
    metas = jnp.stack(metas)
    far = swap(x, 2)
    near = swap(x, 1)

    mark = metas[:, 0].astype(jnp.int32)
    where, s = (mark >> 7) - me * local, mark & 127
    ok = (where >= 0) & (where < local) & (s < slots)
    ids = jnp.arange(local, dtype=jnp.int32)
    is_it = (where[:, None] == ids[None, :, None, None]) & ok[:, None]
    n = jnp.max(jnp.where(is_it, s[:, None] + 1, 0), axis=(2, 3))
    n = (n + ROW - 1) // ROW * ROW
    off = jnp.sum(jnp.where(ids[None, :] < ids[:, None], n[:, None, :], 0), axis=2)
    used = jnp.sum(n, axis=1)
    pos = jnp.where(ok, jnp.sum(jnp.where(is_it, off[:, :, None, None], 0), axis=1) + s, -1).astype(F32)
    nf, of = n.reshape(-1), off.reshape(-1)
    nblk = (used + BLK - 1) // BLK
    k = jnp.maximum((used + DEPTH - 1) // DEPTH, rows // DEPTH - 1)

    def send(q, v):
        return dispatch(nblk[q : q + 1], pos[q], v, rows)

    chunks = s_gate.shape[1] // 512
    cut = chunks * 8 // 11
    y_shared = shared_expert(x, s_gate, s_up, s_down, 0, cut)
    z = [send(0, x), send(1, near)]
    far_near = swap(far, 1)
    comb = combine_matrices(k, pos, metas[:, 1].astype(BF16).astype(F32), rows)
    h = gate_up(nf, of, nblk, w_gate, w_up, [pos[2], pos[3]], [[far], [far_near]], z, most)

    back, kept, at = [], None, 0
    for columns in (d // 2, d // 2):
        y2, y3, kept = down(nf, of, k, w_down, h, comb, kept, at, columns, 2)
        mine = y2 + swap(y3, 1).astype(F32)
        back.append(swap(mine.astype(BF16), 2))
        at += columns
    y1 = side_sums(k, comb, kept, 1)
    side = swap(y1, 1)
    y_shared = shared_expert(x, s_gate, s_up, s_down, cut, chunks, (k, y_shared, comb, kept), rows=256)
    return (y_shared + side.astype(F32) + jnp.concatenate(back, axis=1).astype(F32)).astype(BF16)[None, None]


def solution(mesh):
    members = mesh.shape["ep"]
    tok = P("dp", "ep", None, None)
    w = P("ep", None, None)
    rep = P(None, None)

    def step(x, expert, slot, gate, w_gate, w_up, w_down, s_gate, s_up, s_down):
        body = functools.partial(layer, members=members, experts=w_gate.shape[0])
        return jax.shard_map(
            body,
            mesh=mesh,
            in_specs=(tok, tok, tok, tok, w, w, w, rep, rep, rep),
            out_specs=tok,
            check_vma=False,
        )(x, expert, slot, gate, w_gate, w_up, w_down, s_gate, s_up, s_down)

    return step
```
